256 devices in a mesh: ba: 8 (over z), aa: 32 (over x, y, core).
Axes of the slice: x: 4, y: 4, z: 8, core: 2. Of those that a mesh axis runs over, the one named last changes fastest.
Arguments:
- tokens: bfloat16 [49152, 1024], P(('ba', 'aa')), parts along dimension 0, may hold values from -6 to 6
- latents: bfloat16 [8192, 1024], P(('ba', 'aa')), parts along dimension 0, may hold values from -6 to 6
- read_query: bfloat16 [1024, 512], replicated, may hold values from -0.1875 to 0.1875
- read_keyval: bfloat16 [1024, 1024], replicated, may hold values from -0.1875 to 0.1875
- read_out: bfloat16 [512, 1024], replicated, may hold values from -0.25 to 0.25
- self_qkv: bfloat16 [1024, 1536], replicated, may hold values from -0.1875 to 0.1875
- self_out: bfloat16 [512, 1024], replicated, may hold values from -0.25 to 0.25
- write_query: bfloat16 [1024, 512], replicated, may hold values from -0.1875 to 0.1875
- write_keyval: bfloat16 [1024, 1024], replicated, may hold values from -0.1875 to 0.1875
- write_out: bfloat16 [512, 1024], replicated, may hold values from -0.25 to 0.25
- qk_gain: float32 [6, 512], replicated, may hold values from 0.8 to 2.2
Outputs:
- tokens_out: bfloat16 [49152, 1024], P(('ba', 'aa')), parts along dimension 0
- latents_out: bfloat16 [8192, 1024], P(('ba', 'aa')), parts along dimension 0
The draws below stay inside these ranges and needn't reach their ends.
There are 8 independent parts, one for each index of `ba`. The reference program is written for one: setup_inputs(seed, part) draws one part's arguments, and reference() takes and returns one part's arrays. A program takes and returns all parts, laid end to end along the dimension named above; an argument that names none is the same for every part. Nothing has to cross between parts.
All inputs are finite; a program needn't handle non-finite values.
Results may differ from the reference program's by a relative error of at most 0.014.
Values may be sent and summed in bfloat16 or wider, within the bound.
No kernel may reach another device: no remote copies, remote signals or barrier semaphores. Data moves between devices by JAX's collectives and lax.ppermute only.
A program may use at most 64 MiB of HBM per device.

```python
import math
import jax
import jax.numpy as jnp
from jax import lax

D = 1024
HEADS = 8
INNER = 512
TOKENS = 6144
LATENTS = 1024


def steps_of(own_key, extent, cuts, smallest, largest):
    def one(position, parts):
        steps = jax.random.uniform(jax.random.fold_in(jax.random.fold_in(own_key, 6), position), (parts,), jnp.float32, smallest / len(cuts), largest / len(cuts))
        return jnp.repeat(jnp.exp(steps), extent[position] // parts).reshape((-1,) + (1,) * (len(extent) - position - 1))

    factor_of = one(*cuts[0])
    for cut in cuts[1:]:
        factor_of = factor_of * one(*cut)
    return factor_of


def normal_values(key, extent, width, limit, cuts=(), kind=jnp.bfloat16):
    loudness = steps_of(key, extent, cuts, -0.22, 0.18) if cuts else 1.0
    values = jax.random.normal(key, extent, jnp.float32) * width * loudness
    return jnp.minimum(jnp.maximum(values, -limit), limit).astype(kind)


def setup_inputs(seed: int = 0, part: int = 0) -> dict:
    splits = jax.random.split(jax.random.key(seed), 12)
    own_keys = jax.random.split(jax.random.fold_in(splits[11], part), 12)
    tokens = normal_values(own_keys[0], (TOKENS, D), 1.0, 6.0, ((0, 32),))
    latents = normal_values(own_keys[1], (LATENTS, D), 1.0, 6.0, ((0, 32),))
    read_query = normal_values(splits[2], (D, INNER), D ** -0.5, 0.1875)
    read_keyval = normal_values(splits[3], (D, 2 * INNER), D ** -0.5, 0.1875)
    read_out = normal_values(splits[4], (INNER, D), INNER ** -0.5, 0.25)
    self_qkv = normal_values(splits[5], (D, 3 * INNER), D ** -0.5, 0.1875)
    self_out = normal_values(splits[6], (INNER, D), INNER ** -0.5, 0.25)
    write_query = normal_values(splits[7], (D, INNER), D ** -0.5, 0.1875)
    write_keyval = normal_values(splits[8], (D, 2 * INNER), D ** -0.5, 0.1875)
    write_out = normal_values(splits[9], (INNER, D), INNER ** -0.5, 0.25)
    qk_gain = jnp.clip(jnp.exp(jax.random.uniform(splits[10], (6, INNER), jnp.float32, math.log(0.8), math.log(2.2))), 0.8, 2.2)
    return {"tokens": tokens, "latents": latents, "read_query": read_query, "read_keyval": read_keyval, "read_out": read_out, "self_qkv": self_qkv, "self_out": self_out, "write_query": write_query, "write_keyval": write_keyval, "write_out": write_out, "qk_gain": qk_gain}


EPSILON = 1e-06

def rms_rows(values):
    widened = values.astype(jnp.float32)
    return (widened * lax.rsqrt(lax.optimization_barrier(jnp.mean(widened * widened, axis=-1, keepdims=True)) + EPSILON)).astype(jnp.bfloat16)

def head_norm(projected, gain_row, head_count):
    row_count = projected.shape[0]
    split_heads = projected.reshape(row_count, head_count, -1)
    normed = split_heads * lax.rsqrt(lax.optimization_barrier(jnp.mean(split_heads * split_heads, axis=-1, keepdims=True)) + EPSILON)
    return (normed.reshape(row_count, -1) * gain_row).astype(jnp.bfloat16)

def attend_block(query_rows, key_rows, value_rows, head_count):
    row_count = query_rows.shape[0]
    query_heads = query_rows.reshape(row_count, head_count, -1).astype(jnp.float32)
    key_heads = key_rows.reshape(key_rows.shape[0], head_count, -1).astype(jnp.float32)
    value_heads = value_rows.reshape(value_rows.shape[0], head_count, -1).astype(jnp.float32)
    score_scale = 1.0 / math.sqrt(query_heads.shape[2])
    scores = jnp.einsum('qhe,khe->hqk', query_heads, key_heads) * score_scale
    weights = jnp.exp(scores)
    denominator = lax.optimization_barrier(jnp.sum(weights, axis=2)).T
    rounded = lax.optimization_barrier(weights.astype(jnp.bfloat16)).astype(jnp.float32)
    numerator = jnp.einsum('hqk,khe->qhe', rounded, value_heads)
    quotient = numerator / denominator[:, :, None]
    return quotient.reshape(row_count, -1).astype(jnp.bfloat16)

def attention(query_rows, key_rows, value_rows, head_count):
    row_count = query_rows.shape[0]
    if row_count > 512 and row_count % 512 == 0:
        blocks = query_rows.reshape(row_count // 512, 512, query_rows.shape[1])
        result = lax.map(lambda one_block: attend_block(one_block, key_rows, value_rows, head_count), blocks)
        return result.reshape(row_count, -1)
    return attend_block(query_rows, key_rows, value_rows, head_count)

def residual_add(base, attended, projection):
    update = jnp.dot(attended, projection, preferred_element_type=jnp.float32)
    return (base.astype(jnp.float32) + update).astype(jnp.bfloat16)

def reference(tokens, latents, read_query, read_keyval, read_out, self_qkv, self_out, write_query, write_keyval, write_out, qk_gain):
    inner_width = read_query.shape[1]
    normed_tokens = rms_rows(tokens)
    normed_latents = rms_rows(latents)
    read_queries = head_norm(jnp.dot(normed_latents, read_query, preferred_element_type=jnp.float32), qk_gain[0], HEADS)
    token_pairs = jnp.dot(normed_tokens, read_keyval, preferred_element_type=jnp.float32)
    read_keys = head_norm(token_pairs[:, :inner_width], qk_gain[1], HEADS)
    read_values = token_pairs[:, inner_width:].astype(jnp.bfloat16)
    read_attended = attention(read_queries, read_keys, read_values, HEADS)
    read_latents = residual_add(latents, read_attended, read_out)
    self_normed = rms_rows(read_latents)
    triple = jnp.dot(self_normed, self_qkv, preferred_element_type=jnp.float32)
    self_queries = head_norm(triple[:, :inner_width], qk_gain[2], HEADS)
    self_keys = head_norm(triple[:, inner_width:2 * inner_width], qk_gain[3], HEADS)
    self_values = triple[:, 2 * inner_width:].astype(jnp.bfloat16)
    self_attended = attention(self_queries, self_keys, self_values, HEADS)
    latents_out = residual_add(read_latents, self_attended, self_out)
    write_queries = head_norm(jnp.dot(normed_tokens, write_query, preferred_element_type=jnp.float32), qk_gain[4], HEADS)
    write_normed = rms_rows(latents_out)
    latent_pairs = jnp.dot(write_normed, write_keyval, preferred_element_type=jnp.float32)
    write_keys = head_norm(latent_pairs[:, :inner_width], qk_gain[5], HEADS)
    write_values = latent_pairs[:, inner_width:].astype(jnp.bfloat16)
    write_attended = attention(write_queries, write_keys, write_values, HEADS)
    tokens_out = residual_add(tokens, write_attended, write_out)
    return (tokens_out, latents_out)
```

```python
import math

import jax
import jax.numpy as jnp
from jax import lax
from jax.experimental import pallas as pl
from jax.experimental.pallas import tpu as pltpu
from jax.sharding import Mesh
from jax.sharding import PartitionSpec as P

HEADS = 8
AA = ("aa_0", "aa_1", "aa_2")
BA_AA = ("ba", "aa_0", "aa_1", "aa_2")
EPSILON = 1e-06
QUERY_SCALE = math.log2(math.e) / 8.0
F32, BF16 = jnp.float32, jnp.bfloat16


def low_lanes(shape):
    return lax.broadcasted_iota(jnp.int32, shape, len(shape) - 1) % 128 < 64


def swap(x):
    return pltpu.roll(x, 64, axis=1)


def rms_rows(x):
    return (x * lax.rsqrt(jnp.mean(x * x, axis=-1, keepdims=True) + EPSILON)).astype(BF16)


def head_norm(x, gain):
    row = lax.broadcasted_iota(jnp.int32, (256, 256), 0) // 64
    col = lax.broadcasted_iota(jnp.int32, (256, 256), 1) // 64
    averager = jnp.where(row == col, 1.0 / 64, 0.0).astype(BF16)
    squares = (x * x).astype(BF16)
    means = [
        jnp.dot(squares[:, at : at + 256], averager, preferred_element_type=F32)
        for at in range(0, x.shape[1], 256)
    ]
    return x * lax.rsqrt(jnp.concatenate(means, axis=1) + EPSILON) * gain


def matmul(a, b):
    return jnp.dot(a, b, preferred_element_type=F32)


def matmul_t(a, b):
    return lax.dot_general(a, b, (((1,), (1,)), ((), ())), preferred_element_type=F32)


def pair(x, p):
    return x[:, 128 * p : 128 * (p + 1)]


def key_value_heads(keys, values):
    out = []
    for p in range(HEADS // 2):
        k, v = pair(keys, p), pair(values, p)
        low = low_lanes(k.shape)
        out.append(jnp.where(low, k, swap(v)).astype(BF16))
        out.append(jnp.where(low, swap(k), v).astype(BF16))
    return out


def query_heads(queries):
    half = queries.shape[0] // 2
    out = []
    for p in range(HEADS // 2):
        q = pair(queries, p)
        s = swap(q)
        low = low_lanes((half, 128))
        out.append(jnp.where(low, q[:half], s[half:]).astype(BF16))
        out.append(jnp.where(low, s[:half], q[half:]).astype(BF16))
    return out


def with_ones(kv, low):
    return jnp.where(low, jnp.ones_like(kv), kv)


def project_kernel(
    tokens_ref, latents_ref, wq_ref, wkv_ref, wwq_ref, gain_ref, send_ref, keep_ref, give_ref
):
    normed = rms_rows(tokens_ref[...].astype(F32))
    kv = matmul(normed, wkv_ref[...])
    keys = head_norm(kv[:, :512], gain_ref[1:2, :])
    groups = send_ref.shape[0] // HEADS
    count = kv.shape[0] // groups
    for h, block in enumerate(key_value_heads(keys, kv[:, 512:])):
        for g in range(groups):
            send_ref[g * HEADS + h, :count, :] = block[g * count : (g + 1) * count]
    queries = matmul(rms_rows(latents_ref[...].astype(F32)), wq_ref[...])
    queries = head_norm(queries, gain_ref[0:1, :] * QUERY_SCALE)
    for h, block in enumerate(query_heads(queries)):
        for g in range(groups):
            send_ref[g * HEADS + h, count:, :] = block
    writes = head_norm(matmul(normed, wwq_ref[...]), gain_ref[4:5, :] * QUERY_SCALE)
    first = lax.axis_index("aa_2") == 0
    low, high = writes[:, :256], writes[:, 256:]
    keep_ref[...] = jnp.where(first, low, high).astype(BF16)
    give_ref[...] = jnp.where(first, high, low).astype(BF16)


def read_kernel(got_ref, out_ref):
    devices, rows, _ = got_ref.shape
    count = rows - 16
    kv = got_ref[:, :count, :].reshape(devices * count, 128)
    kv1 = with_ones(kv, low_lanes(kv.shape))
    step = 16
    for at in range(0, devices, step):
        packed = got_ref[at : at + step, count:, :].reshape(step * 16, 128).astype(F32)
        low = low_lanes(packed.shape)
        for half, q in enumerate((packed, swap(packed))):
            q = jnp.where(low, q, 0.0).astype(BF16)
            weights = jnp.exp2(matmul_t(q, kv)).astype(BF16)
            o = matmul(weights, kv1)
            out_ref[at : at + step, half * 16 : half * 16 + 16, :] = o.astype(BF16).reshape(
                step, 16, 128
            )


def self_project_kernel(got_ref, latents_ref, wo_ref, wqkv_ref, gain_ref, rows_ref, send_ref):
    devices = got_ref.shape[0]
    groups = devices // HEADS
    blocks = []
    for p in range(HEADS // 2):
        both = []
        for h in (2 * p, 2 * p + 1):
            total = got_ref[h].astype(F32)
            for g in range(1, groups):
                total = total + got_ref[g * HEADS + h].astype(F32)
            both.append(total / swap(total))
        blocks.append(jnp.where(low_lanes(both[0].shape), swap(both[0]), both[1]).astype(BF16))
    attended = jnp.concatenate(blocks, axis=1)
    rows = (latents_ref[...].astype(F32) + matmul(attended, wo_ref[...])).astype(BF16)
    rows_ref[...] = rows
    triple = matmul(rms_rows(rows.astype(F32)), wqkv_ref[...])
    queries = head_norm(triple[:, :512], gain_ref[2:3, :] * QUERY_SCALE)
    keys = head_norm(triple[:, 512:1024], gain_ref[3:4, :])
    count = rows.shape[0]
    kv_blocks = key_value_heads(keys, triple[:, 1024:])
    for h, (kv, q) in enumerate(zip(kv_blocks, query_heads(queries))):
        for g in range(groups):
            send_ref[g * HEADS + h, :count, :] = kv
            send_ref[g * HEADS + h, count:, :] = q


def self_kernel(got_ref, out_ref):
    devices, rows, _ = got_ref.shape
    count = rows - 16
    kv = got_ref[:, :count, :].reshape(devices * count, 128)
    kv1 = with_ones(kv, low_lanes(kv.shape))
    mine = lax.axis_index("aa_0") * HEADS
    packed = got_ref[pl.ds(mine, HEADS), count:, :].reshape(HEADS * 16, 128).astype(F32)
    low = low_lanes(packed.shape)
    outs = []
    for q in (packed, swap(packed)):
        q = jnp.where(low, q, 0.0).astype(BF16)
        weights = jnp.exp2(matmul_t(q, kv)).astype(BF16)
        o = matmul(weights, kv1)
        outs.append(o / swap(o))
    out_ref[...] = jnp.where(low, swap(outs[0]), outs[1]).astype(BF16).reshape(HEADS, 16, 128)


def write_project_kernel(got_ref, rows_ref, wo_ref, wkv_ref, gain_ref, latents_ref, send_ref):
    blocks = []
    for p in range(HEADS // 2):
        e, o = got_ref[2 * p].astype(F32), got_ref[2 * p + 1].astype(F32)
        low = low_lanes(e.shape)
        top, bottom = jnp.where(low, e, swap(o)), jnp.where(low, swap(e), o)
        blocks.append(jnp.concatenate([top, bottom], axis=0).astype(BF16))
    attended = jnp.concatenate(blocks, axis=1)
    rows = (rows_ref[...].astype(F32) + matmul(attended, wo_ref[...])).astype(BF16)
    latents_ref[...] = rows
    kv = matmul(rms_rows(rows.astype(F32)), wkv_ref[...])
    keys, values = head_norm(kv[:, :512], gain_ref[5:6, :]), kv[:, 512:]
    for p in range(HEADS // 2):
        k, v = pair(keys, p), swap(pair(values, p))
        low = low_lanes(k.shape)
        even = jnp.where(low, k, v).astype(BF16)
        odd = jnp.where(low, v, k).astype(BF16)
        core, at = p // 2, 256 * (p % 2)
        for chip in range(send_ref.shape[0] // 2):
            send_ref[2 * chip + core, :, at : at + 128] = even
            send_ref[2 * chip + core, :, at + 128 : at + 256] = odd


def write_kernel(q_ref, got_ref, out_ref):
    devices, rows, _ = got_ref.shape
    for p in range(2):
        q = q_ref[:, 128 * p : 128 * (p + 1)]
        low = low_lanes(q.shape)
        results = []
        for odd in (0, 1):
            at = 128 * (2 * p + odd)
            kv = got_ref[:, :, at : at + 128].reshape(devices * rows, 128)
            keyed = low_lanes(kv.shape)
            if odd:
                keyed, used = jnp.logical_not(keyed), jnp.where(low, jnp.zeros_like(q), q)
            else:
                used = jnp.where(low, q, jnp.zeros_like(q))
            weights = jnp.exp2(matmul_t(used, kv)).astype(BF16)
            o = matmul(weights, with_ones(kv, keyed))
            results.append(o / swap(o))
        even, odd = results
        out_ref[:, 128 * p : 128 * (p + 1)] = swap(jnp.where(low, odd, even)).astype(BF16)


def finish_kernel(tokens_ref, mine_ref, other_ref, wo_ref, out_ref):
    core = lax.axis_index("aa_2")
    own = wo_ref[pl.ds(pl.multiple_of(core * 256, 256), 256), :]
    rest = wo_ref[pl.ds(pl.multiple_of((1 - core) * 256, 256), 256), :]
    update = matmul(mine_ref[...], own) + matmul(other_ref[...], rest)
    out_ref[...] = (tokens_ref[...].astype(F32) + update).astype(BF16)


def call(body, outs, *args, flops=0):
    shapes = tuple(jax.ShapeDtypeStruct(s, BF16) for s in outs)
    return pl.pallas_call(
        body,
        out_shape=shapes if len(shapes) > 1 else shapes[0],
        in_specs=[pl.BlockSpec(memory_space=pltpu.VMEM)] * len(args),
        out_specs=tuple(pl.BlockSpec(memory_space=pltpu.VMEM) for _ in shapes)
        if len(shapes) > 1
        else pl.BlockSpec(memory_space=pltpu.VMEM),
        compiler_params=pltpu.CompilerParams(vmem_limit_bytes=48 * 1024 * 1024),
        cost_estimate=pl.CostEstimate(
            flops=flops,
            transcendentals=0,
            bytes_accessed=sum(a.size * a.dtype.itemsize for a in args),
        ),
    )(*args)


def all_to_all(x, axes):
    return lax.all_to_all(x, axes, split_axis=0, concat_axis=0, tiled=True)


def per_device(
    tokens,
    latents,
    read_query,
    read_keyval,
    read_out,
    self_qkv,
    self_out,
    write_query,
    write_keyval,
    write_out,
    qk_gain,
):
    count, rows = tokens.shape[0], latents.shape[0]
    devices = lax.axis_size(AA)
    groups = devices // HEADS
    other_core = [(0, 1), (1, 0)]
    sent, keep, give = call(
        project_kernel,
        ((devices, count // groups + 16, 128), (count, 256), (count, 256)),
        tokens,
        latents,
        read_query,
        read_keyval,
        write_query,
        qk_gain,
        flops=10**9,
    )
    taken = lax.ppermute(give, "aa_2", other_core)
    got = all_to_all(sent, AA)
    partial = call(read_kernel, ((devices, rows, 128),), got, flops=10**9)
    partial = all_to_all(partial, AA)
    own_rows, sent = call(
        self_project_kernel,
        ((rows, 1024), (devices, rows + 16, 128)),
        partial,
        latents,
        read_out,
        self_qkv,
        qk_gain,
        flops=10**9,
    )
    got = all_to_all(sent, AA)
    attended = call(self_kernel, ((HEADS, 16, 128),), got, flops=10**9)
    attended = all_to_all(attended, ("aa_1", "aa_2"))
    latents_out, sent = call(
        write_project_kernel,
        ((rows, 1024), (devices, rows, 512)),
        attended,
        own_rows,
        self_out,
        write_keyval,
        qk_gain,
        flops=10**9,
    )
    got = all_to_all(sent, AA)
    theirs = call(write_kernel, ((count, 256),), taken, got, flops=10**9)
    other = lax.ppermute(theirs, "aa_2", other_core)
    mine = call(write_kernel, ((count, 256),), keep, got, flops=10**9)
    tokens_out = call(
        finish_kernel, ((count, 1024),), tokens, mine, other, write_out, flops=10**9
    )
    return (tokens_out, latents_out)


def solution(mesh):
    torus = Mesh(mesh.devices.reshape(mesh.shape["ba"], 4, 4, 2), ("ba", "aa_0", "aa_1", "aa_2"))
    in_specs = (P(BA_AA, None), P(BA_AA, None), P(), P(), P(), P(), P(), P(), P(), P(), P())
    out_specs = (P(BA_AA, None), P(BA_AA, None))
    return jax.shard_map(
        per_device, mesh=torus, in_specs=in_specs, out_specs=out_specs, check_vma=False
    )
```

```python
import math

import jax
import jax.numpy as jnp
from jax import lax
from jax.experimental import pallas as pl
from jax.experimental.pallas import tpu as pltpu
from jax.sharding import Mesh
from jax.sharding import PartitionSpec as P

HEADS = 8
AA = ("aa_0", "aa_1", "aa_2")
BA_AA = ("ba", "aa_0", "aa_1", "aa_2")
EPSILON = 1e-06
QUERY_SCALE = math.log2(math.e) / 8.0
F32, BF16 = jnp.float32, jnp.bfloat16


def low_lanes(shape):
    return lax.broadcasted_iota(jnp.int32, shape, len(shape) - 1) % 128 < 64


def swap(x):
    return pltpu.roll(x, 64, axis=1)


def rms_rows(x):
    return (x * lax.rsqrt(jnp.mean(x * x, axis=-1, keepdims=True) + EPSILON)).astype(BF16)


def head_norm(x, gain):
    row = lax.broadcasted_iota(jnp.int32, (256, 256), 0) // 64
    col = lax.broadcasted_iota(jnp.int32, (256, 256), 1) // 64
    averager = jnp.where(row == col, 1.0 / 64, 0.0).astype(BF16)
    squares = (x * x).astype(BF16)
    means = [
        jnp.dot(squares[:, at : at + 256], averager, preferred_element_type=F32)
        for at in range(0, x.shape[1], 256)
    ]
    return x * lax.rsqrt(jnp.concatenate(means, axis=1) + EPSILON) * gain


def matmul(a, b):
    return jnp.dot(a, b, preferred_element_type=F32)


def matmul_t(a, b):
    return lax.dot_general(a, b, (((1,), (1,)), ((), ())), preferred_element_type=F32)


def pair(x, p):
    return x[:, 128 * p : 128 * (p + 1)]


def key_value_heads(keys, values):
    out = []
    for p in range(HEADS // 2):
        k, v = pair(keys, p), pair(values, p)
        low = low_lanes(k.shape)
        out.append(jnp.where(low, k, swap(v)).astype(BF16))
        out.append(jnp.where(low, swap(k), v).astype(BF16))
    return out


def query_heads(queries):
    half = queries.shape[0] // 2
    out = []
    for p in range(HEADS // 2):
        q = pair(queries, p)
        s = swap(q)
        low = low_lanes((half, 128))
        out.append(jnp.where(low, q[:half], s[half:]).astype(BF16))
        out.append(jnp.where(low, s[:half], q[half:]).astype(BF16))
    return out


def with_ones(kv, low):
    return jnp.where(low, jnp.ones_like(kv), kv)


def project_kernel(
    tokens_hbm,
    latents_hbm,
    wq_hbm,
    wkv_hbm,
    gain_hbm,
    send_ref,
    tokens_ref,
    latents_ref,
    wq_ref,
    wkv_ref,
    gain_ref,
    sems,
):
    half = wkv_ref.shape[1] // 2
    copies = [
        pltpu.make_async_copy(src, dst, sems.at[i])
        for i, (src, dst) in enumerate(
            (
                (gain_hbm, gain_ref),
                (latents_hbm, latents_ref),
                (tokens_hbm, tokens_ref),
                (wq_hbm, wq_ref),
                (wkv_hbm.at[:, :half], wkv_ref.at[:, :half]),
                (wkv_hbm.at[:, half:], wkv_ref.at[:, half:]),
            )
        )
    ]
    for copy in copies:
        copy.start()
    groups = send_ref.shape[0] // HEADS
    count = tokens_ref.shape[0] // groups
    copies[0].wait()
    copies[1].wait()
    latents = rms_rows(latents_ref[...].astype(F32))
    copies[2].wait()
    normed = rms_rows(tokens_ref[...].astype(F32))
    copies[3].wait()
    queries = head_norm(matmul(latents, wq_ref[...]), gain_ref[0:1, :] * QUERY_SCALE)
    for h, block in enumerate(query_heads(queries)):
        for g in range(groups):
            send_ref[g * HEADS + h, count:, :] = block
    copies[4].wait()
    keys = head_norm(matmul(normed, wkv_ref[:, :half]), gain_ref[1:2, :])
    copies[5].wait()
    values = matmul(normed, wkv_ref[:, half:])
    for h, block in enumerate(key_value_heads(keys, values)):
        for g in range(groups):
            send_ref[g * HEADS + h, :count, :] = block[g * count : (g + 1) * count]


def write_query_kernel(tokens_ref, wwq_ref, gain_ref, keep_ref, give_ref):
    normed = rms_rows(tokens_ref[...].astype(F32))
    writes = head_norm(matmul(normed, wwq_ref[...]), gain_ref[4:5, :] * QUERY_SCALE)
    first = lax.axis_index("aa_2") == 0
    low, high = writes[:, :256], writes[:, 256:]
    keep_ref[...] = jnp.where(first, low, high).astype(BF16)
    give_ref[...] = jnp.where(first, high, low).astype(BF16)


def read_kernel(got_ref, out_ref):
    devices, rows, _ = got_ref.shape
    count = rows - 16
    kv = got_ref[:, :count, :].reshape(devices * count, 128)
    kv1 = with_ones(kv, low_lanes(kv.shape))
    step = 16
    for at in range(0, devices, step):
        packed = got_ref[at : at + step, count:, :].reshape(step * 16, 128).astype(F32)
        low = low_lanes(packed.shape)
        for half, q in enumerate((packed, swap(packed))):
            q = jnp.where(low, q, 0.0).astype(BF16)
            weights = jnp.exp2(matmul_t(q, kv)).astype(BF16)
            o = matmul(weights, kv1)
            out_ref[at : at + step, half * 16 : half * 16 + 16, :] = o.astype(BF16).reshape(
                step, 16, 128
            )


def self_project_kernel(got_ref, latents_ref, wo_ref, wqkv_ref, gain_ref, rows_ref, send_ref):
    devices = got_ref.shape[0]
    groups = devices // HEADS
    blocks = []
    for p in range(HEADS // 2):
        both = []
        for h in (2 * p, 2 * p + 1):
            total = got_ref[h].astype(F32)
            for g in range(1, groups):
                total = total + got_ref[g * HEADS + h].astype(F32)
            both.append(total / swap(total))
        blocks.append(jnp.where(low_lanes(both[0].shape), swap(both[0]), both[1]).astype(BF16))
    attended = jnp.concatenate(blocks, axis=1)
    rows = (latents_ref[...].astype(F32) + matmul(attended, wo_ref[...])).astype(BF16)
    rows_ref[...] = rows
    triple = matmul(rms_rows(rows.astype(F32)), wqkv_ref[...])
    queries = head_norm(triple[:, :512], gain_ref[2:3, :] * QUERY_SCALE)
    keys = head_norm(triple[:, 512:1024], gain_ref[3:4, :])
    count = rows.shape[0]
    kv_blocks = key_value_heads(keys, triple[:, 1024:])
    for h, (kv, q) in enumerate(zip(kv_blocks, query_heads(queries))):
        for g in range(groups):
            send_ref[g * HEADS + h, :count, :] = kv
            send_ref[g * HEADS + h, count:, :] = q


def self_kernel(got_ref, out_ref):
    devices, rows, _ = got_ref.shape
    count = rows - 16
    kv = got_ref[:, :count, :].reshape(devices * count, 128)
    kv1 = with_ones(kv, low_lanes(kv.shape))
    mine = lax.axis_index("aa_0") * HEADS
    packed = got_ref[pl.ds(mine, HEADS), count:, :].reshape(HEADS * 16, 128).astype(F32)
    low = low_lanes(packed.shape)
    outs = []
    for q in (packed, swap(packed)):
        q = jnp.where(low, q, 0.0).astype(BF16)
        weights = jnp.exp2(matmul_t(q, kv)).astype(BF16)
        o = matmul(weights, kv1)
        outs.append(o / swap(o))
    out_ref[...] = jnp.where(low, swap(outs[0]), outs[1]).astype(BF16).reshape(HEADS, 16, 128)


def write_project_kernel(got_ref, rows_ref, wo_ref, wkv_ref, gain_ref, latents_ref, send_ref):
    blocks = []
    for p in range(HEADS // 2):
        e, o = got_ref[2 * p].astype(F32), got_ref[2 * p + 1].astype(F32)
        low = low_lanes(e.shape)
        top, bottom = jnp.where(low, e, swap(o)), jnp.where(low, swap(e), o)
        blocks.append(jnp.concatenate([top, bottom], axis=0).astype(BF16))
    attended = jnp.concatenate(blocks, axis=1)
    rows = (rows_ref[...].astype(F32) + matmul(attended, wo_ref[...])).astype(BF16)
    latents_ref[...] = rows
    kv = matmul(rms_rows(rows.astype(F32)), wkv_ref[...])
    keys, values = head_norm(kv[:, :512], gain_ref[5:6, :]), kv[:, 512:]
    for p in range(HEADS // 2):
        k, v = pair(keys, p), swap(pair(values, p))
        low = low_lanes(k.shape)
        even = jnp.where(low, k, v).astype(BF16)
        odd = jnp.where(low, v, k).astype(BF16)
        core, at = p // 2, 256 * (p % 2)
        for chip in range(send_ref.shape[0] // 2):
            send_ref[2 * chip + core, :, at : at + 128] = even
            send_ref[2 * chip + core, :, at + 128 : at + 256] = odd


def write_kernel(q_ref, got_ref, out_ref):
    devices, rows, _ = got_ref.shape
    for p in range(2):
        q = q_ref[:, 128 * p : 128 * (p + 1)]
        low = low_lanes(q.shape)
        results = []
        for odd in (0, 1):
            at = 128 * (2 * p + odd)
            kv = got_ref[:, :, at : at + 128].reshape(devices * rows, 128)
            keyed = low_lanes(kv.shape)
            if odd:
                keyed, used = jnp.logical_not(keyed), jnp.where(low, jnp.zeros_like(q), q)
            else:
                used = jnp.where(low, q, jnp.zeros_like(q))
            weights = jnp.exp2(matmul_t(used, kv)).astype(BF16)
            o = matmul(weights, with_ones(kv, keyed))
            results.append(o / swap(o))
        even, odd = results
        out_ref[:, 128 * p : 128 * (p + 1)] = swap(jnp.where(low, odd, even)).astype(BF16)


def finish_kernel(tokens_ref, mine_ref, other_ref, wo_ref, out_ref):
    core = lax.axis_index("aa_2")
    own = wo_ref[pl.ds(pl.multiple_of(core * 256, 256), 256), :]
    rest = wo_ref[pl.ds(pl.multiple_of((1 - core) * 256, 256), 256), :]
    update = matmul(mine_ref[...], own) + matmul(other_ref[...], rest)
    out_ref[...] = (tokens_ref[...].astype(F32) + update).astype(BF16)


def call(body, outs, *args, flops=0, fetch=False):
    space = pltpu.HBM if fetch else pltpu.VMEM
    scratch = [pltpu.VMEM(a.shape, a.dtype) for a in args] if fetch else []
    if fetch:
        scratch.append(pltpu.SemaphoreType.DMA((len(args) + 1,)))
        args = [pltpu.with_memory_space_constraint(a, space) for a in args]
    shapes = tuple(jax.ShapeDtypeStruct(s, BF16) for s in outs)
    return pl.pallas_call(
        body,
        out_shape=shapes if len(shapes) > 1 else shapes[0],
        in_specs=[pl.BlockSpec(memory_space=space)] * len(args),
        scratch_shapes=scratch,
        out_specs=tuple(pl.BlockSpec(memory_space=pltpu.VMEM) for _ in shapes)
        if len(shapes) > 1
        else pl.BlockSpec(memory_space=pltpu.VMEM),
        compiler_params=pltpu.CompilerParams(vmem_limit_bytes=48 * 1024 * 1024),
        cost_estimate=pl.CostEstimate(
            flops=flops,
            transcendentals=0,
            bytes_accessed=sum(a.size * a.dtype.itemsize for a in args),
        ),
    )(*args)


def all_to_all(x, axes):
    return lax.all_to_all(x, axes, split_axis=0, concat_axis=0, tiled=True)


def per_device(
    tokens,
    latents,
    read_query,
    read_keyval,
    read_out,
    self_qkv,
    self_out,
    write_query,
    write_keyval,
    write_out,
    qk_gain,
):
    count, rows = tokens.shape[0], latents.shape[0]
    devices = lax.axis_size(AA)
    groups = devices // HEADS
    other_core = [(0, 1), (1, 0)]
    sent = call(
        project_kernel,
        ((devices, count // groups + 16, 128),),
        tokens,
        latents,
        read_query,
        read_keyval,
        qk_gain,
        flops=10**9,
        fetch=True,
    )
    got = all_to_all(sent, AA)
    partial = call(read_kernel, ((devices, rows, 128),), got, flops=10**9)
    partial = all_to_all(partial, AA)
    own_rows, sent = call(
        self_project_kernel,
        ((rows, 1024), (devices, rows + 16, 128)),
        partial,
        latents,
        read_out,
        self_qkv,
        qk_gain,
        flops=10**9,
    )
    got = all_to_all(sent, AA)
    attended = call(self_kernel, ((HEADS, 16, 128),), got, flops=10**9)
    attended = all_to_all(attended, ("aa_1", "aa_2"))
    latents_out, sent = call(
        write_project_kernel,
        ((rows, 1024), (devices, rows, 512)),
        attended,
        own_rows,
        self_out,
        write_keyval,
        qk_gain,
        flops=10**9,
    )
    got = all_to_all(sent, AA)
    keep, give = call(
        write_query_kernel,
        ((count, 256), (count, 256)),
        tokens,
        write_query,
        qk_gain,
        flops=10**9,
    )
    taken = lax.ppermute(give, "aa_2", other_core)
    theirs = call(write_kernel, ((count, 256),), taken, got, flops=10**9)
    other = lax.ppermute(theirs, "aa_2", other_core)
    mine = call(write_kernel, ((count, 256),), keep, got, flops=10**9)
    tokens_out = call(
        finish_kernel, ((count, 1024),), tokens, mine, other, write_out, flops=10**9
    )
    return (tokens_out, latents_out)


def solution(mesh):
    torus = Mesh(mesh.devices.reshape(mesh.shape["ba"], 4, 4, 2), ("ba", "aa_0", "aa_1", "aa_2"))
    in_specs = (P(BA_AA, None), P(BA_AA, None), P(), P(), P(), P(), P(), P(), P(), P(), P())
    out_specs = (P(BA_AA, None), P(BA_AA, None))
    return jax.shard_map(
        per_device, mesh=torus, in_specs=in_specs, out_specs=out_specs, check_vma=False
    )
```

```python
import math

import jax
import jax.numpy as jnp
from jax import lax
from jax.experimental import pallas as pl
from jax.experimental.pallas import tpu as pltpu
from jax.sharding import Mesh
from jax.sharding import PartitionSpec as P

AA = ("aa_0", "aa_1", "aa_2")
BA_AA = ("ba", "aa_0", "aa_1", "aa_2")
PAIRS = 4
EPSILON = 1e-06
QUERY_SCALE = math.log2(math.e) / 8.0
F32, BF16 = jnp.float32, jnp.bfloat16


def own_pair():
    return 2 * lax.rem(lax.axis_index("aa_1"), 2) + lax.axis_index("aa_2")


def to_peer(x, k):
    swaps = [(i, i ^ k) for i in range(8)]
    return lax.ppermute(x, ("aa_1", "aa_2"), swaps)


def low_lanes(shape):
    return lax.broadcasted_iota(jnp.int32, shape, len(shape) - 1) < 64


def rms_rows(x):
    return (x * lax.rsqrt(jnp.mean(x * x, axis=-1, keepdims=True) + EPSILON)).astype(BF16)


def matmul(a, b):
    return jnp.dot(a, b, preferred_element_type=F32)


def matmul_t(a, b):
    return lax.dot_general(a, b, (((1,), (1,)), ((), ())), preferred_element_type=F32)


def head_norm(x, gain):
    row = lax.broadcasted_iota(jnp.int32, (256, 256), 0) // 64
    col = lax.broadcasted_iota(jnp.int32, (256, 256), 1) // 64
    averager = jnp.where(row == col, 1.0 / 64, 0.0).astype(BF16)
    squares = (x * x).astype(BF16)
    means = [matmul(squares[:, at : at + 256], averager) for at in range(0, x.shape[1], 256)]
    return (x * lax.rsqrt(jnp.concatenate(means, axis=1) + EPSILON) * gain).astype(BF16)


def pair_of(x, p):
    return x[:, 128 * p : 128 * (p + 1)]


def attend(q, k, v):
    low = low_lanes(q.shape)
    values_low = low_lanes(v.shape)
    zero, one = jnp.zeros_like(q), jnp.ones_like(v)
    even = jnp.exp2(matmul_t(jnp.where(low, q, zero), k)).astype(BF16)
    odd = jnp.exp2(matmul_t(jnp.where(low, zero, q), k)).astype(BF16)
    even = matmul(even, jnp.where(values_low, v, one))
    odd = matmul(odd, jnp.where(values_low, one, v))
    return jnp.where(low, even, odd), jnp.where(low, odd, even)


def attend_whole(q, k, v):
    numerator, crossed = attend(q, k, v)
    return (numerator / pltpu.roll(crossed, 64, axis=1)).astype(BF16)


def fetched(sources, targets, sems):
    copies = [
        pltpu.make_async_copy(s, t, sems.at[i]) for i, (s, t) in enumerate(zip(sources, targets))
    ]
    for copy in copies:
        copy.start()
    return copies


def hand_out(blocks_ref, outs):
    mine = own_pair()
    for k, out in enumerate(outs):
        out[...] = blocks_ref[mine ^ k]


def read_query_kernel(latents_hbm, wq_hbm, gain_hbm, send_ref, latents_ref, wq_ref, gain_ref, sems):
    first, second, third = fetched(
        (latents_hbm, wq_hbm, gain_hbm), (latents_ref, wq_ref, gain_ref), sems
    )
    first.wait()
    normed = rms_rows(latents_ref[...].astype(F32))
    second.wait()
    third.wait()
    queries = head_norm(matmul(normed, wq_ref[...]), gain_ref[0:1, :] * QUERY_SCALE)
    for d in range(send_ref.shape[0]):
        send_ref[d] = pair_of(queries, d % PAIRS)


def read_keyval_kernel(tokens_ref, wkv_ref, gain_ref, o0, o1, o2, o3, blocks_ref):
    count = tokens_ref.shape[0]
    normed = rms_rows(tokens_ref[...].astype(F32))
    keys = head_norm(matmul(normed, wkv_ref[:, :512]), gain_ref[1:2, :])
    values = matmul(normed, wkv_ref[:, 512:]).astype(BF16)
    for p in range(PAIRS):
        blocks_ref[p, :count] = pair_of(keys, p)
        blocks_ref[p, count:] = pair_of(values, p)
    hand_out(blocks_ref, (o0, o1, o2, o3))


def write_query_kernel(tokens_ref, wwq_ref, gain_ref, o0, o1, o2, o3, blocks_ref):
    normed = rms_rows(tokens_ref[...].astype(F32))
    queries = head_norm(matmul(normed, wwq_ref[...]), gain_ref[4:5, :] * QUERY_SCALE)
    for p in range(PAIRS):
        blocks_ref[p] = pair_of(queries, p)
    hand_out(blocks_ref, (o0, o1, o2, o3))


def read_kernel(got_ref, r0, r1, r2, r3, out_ref):
    devices, rows, _ = got_ref.shape
    count = r0.shape[0] // 2
    k = jnp.concatenate([r[:count] for r in (r0, r1, r2, r3)], axis=0)
    v = jnp.concatenate([r[count:] for r in (r0, r1, r2, r3)], axis=0)
    step = 8
    for at in range(0, devices, step):
        q = got_ref[at : at + step].reshape(step * rows, 128)
        numerator, crossed = attend(q, k, v)
        out_ref[at : at + step, :rows] = numerator.astype(BF16).reshape(step, rows, 128)
        crossed = crossed.reshape(step, rows // 8, 8, 128)
        part = lax.broadcasted_iota(jnp.int32, (step, 8, 128), 2) // 16 % 4
        packed = crossed[:, 0]
        for j in range(1, 4):
            packed = jnp.where(part == j, crossed[:, j], packed)
        out_ref[at : at + step, rows:] = packed.astype(BF16)


def self_project_kernel(
    got_ref, latents_ref, wo_ref, wqkv_ref, gain_ref, rows_ref, send_ref, q0, q1, q2, q3, blocks_ref
):
    devices = got_ref.shape[0]
    count = latents_ref.shape[0]
    quads = devices // PAIRS
    part = lax.broadcasted_iota(jnp.int32, (8, 128), 1) // 16 % 4
    row = lax.broadcasted_iota(jnp.int32, (128 * quads, 128), 0) % 128 // 64
    col = lax.broadcasted_iota(jnp.int32, (128 * quads, 128), 1) // 64
    spread = jnp.where(row == col, 0.0, 1.0 / 16).astype(BF16)
    attended = []
    for p in range(PAIRS):
        numerator = got_ref[p, :count].astype(F32)
        for g in range(1, quads):
            numerator = numerator + got_ref[g * PAIRS + p, :count].astype(F32)
        packed = [got_ref[g * PAIRS + p, count:] for g in range(quads)]
        unpacked = [
            jnp.concatenate(
                [jnp.where(part == j, x.astype(F32), 0.0) for j in range(4)], axis=0
            ).astype(BF16)
            for x in packed
        ]
        denominator = matmul(jnp.concatenate(unpacked, axis=1), spread)
        attended.append((numerator / denominator).astype(BF16))
    attended = jnp.concatenate(attended, axis=1)
    rows = (latents_ref[...].astype(F32) + matmul(attended, wo_ref[...])).astype(BF16)
    rows_ref[...] = rows
    triple = matmul(rms_rows(rows.astype(F32)), wqkv_ref[...])
    queries = head_norm(triple[:, :512], gain_ref[2:3, :] * QUERY_SCALE)
    keys = head_norm(triple[:, 512:1024], gain_ref[3:4, :])
    values = triple[:, 1024:].astype(BF16)
    for p in range(PAIRS):
        blocks_ref[p] = pair_of(queries, p)
    for d in range(devices):
        send_ref[d, :count] = pair_of(keys, d % PAIRS)
        send_ref[d, count:] = pair_of(values, d % PAIRS)
    hand_out(blocks_ref, (q0, q1, q2, q3))


def keys_of(got_ref):
    devices, rows, _ = got_ref.shape
    return got_ref[:, : rows // 2].reshape(devices * rows // 2, 128)


def values_of(got_ref):
    devices, rows, _ = got_ref.shape
    return got_ref[:, rows // 2 :].reshape(devices * rows // 2, 128)


def attend_kernel(got_ref, *refs):
    queries, outs = refs[: len(refs) // 2], refs[len(refs) // 2 :]
    count = queries[0].shape[0]
    q = jnp.concatenate([q[...] for q in queries], axis=0)
    result = attend_whole(q, keys_of(got_ref), values_of(got_ref))
    for i, out in enumerate(outs):
        out[...] = result[i * count : (i + 1) * count]


def gathered(blocks_ref, parts):
    mine = own_pair()
    for k, part in enumerate(parts):
        blocks_ref[mine ^ k] = part[...]
    return jnp.concatenate([blocks_ref[p] for p in range(PAIRS)], axis=1)


def write_project_kernel(
    a0, a1, a2, a3, rows_ref, wo_ref, wkv_ref, gain_ref, latents_ref, send_ref, blocks_ref
):
    attended = gathered(blocks_ref, (a0, a1, a2, a3))
    rows = (rows_ref[...].astype(F32) + matmul(attended, wo_ref[...])).astype(BF16)
    latents_ref[...] = rows
    count = rows.shape[0]
    kv = matmul(rms_rows(rows.astype(F32)), wkv_ref[...])
    keys = head_norm(kv[:, :512], gain_ref[5:6, :])
    values = kv[:, 512:].astype(BF16)
    for d in range(send_ref.shape[0]):
        send_ref[d, :count] = pair_of(keys, d % PAIRS)
        send_ref[d, count:] = pair_of(values, d % PAIRS)


def finish_kernel(a0, a1, a2, a3, tokens_ref, wo_ref, out_ref, blocks_ref):
    update = matmul(gathered(blocks_ref, (a0, a1, a2, a3)), wo_ref[...])
    out_ref[...] = (tokens_ref[...].astype(F32) + update).astype(BF16)


def call(body, outs, *args, scratch=(), fetch=False):
    space = pltpu.HBM if fetch else pltpu.VMEM
    scratch = list(scratch)
    if fetch:
        scratch += [pltpu.VMEM(a.shape, a.dtype) for a in args]
        scratch.append(pltpu.SemaphoreType.DMA((len(args),)))
        args = [pltpu.with_memory_space_constraint(a, space) for a in args]
    results = pl.pallas_call(
        body,
        out_shape=tuple(jax.ShapeDtypeStruct(s, BF16) for s in outs),
        in_specs=[pl.BlockSpec(memory_space=space)] * len(args),
        out_specs=tuple(pl.BlockSpec(memory_space=pltpu.VMEM) for _ in outs),
        scratch_shapes=scratch,
        compiler_params=pltpu.CompilerParams(vmem_limit_bytes=48 * 1024 * 1024),
        cost_estimate=pl.CostEstimate(
            flops=10**9,
            transcendentals=0,
            bytes_accessed=sum(a.size * a.dtype.itemsize for a in args),
        ),
    )(*args)
    return results if len(outs) > 1 else results[0]


def blocks(rows):
    return [pltpu.VMEM((PAIRS, rows, 128), BF16)]


def all_to_all(x):
    return lax.all_to_all(x, AA, split_axis=0, concat_axis=0, tiled=True)


def swapped(parts):
    there = {k: to_peer(parts[k], k) for k in (3, 2, 1)}
    return (parts[0], there[1], there[2], there[3])


def per_device(
    tokens,
    latents,
    read_query,
    read_keyval,
    read_out,
    self_qkv,
    self_out,
    write_query,
    write_keyval,
    write_out,
    qk_gain,
):
    count, rows = tokens.shape[0], latents.shape[0]
    devices = lax.axis_size(AA)
    sent = call(
        read_query_kernel, ((devices, rows, 128),), latents, read_query, qk_gain, fetch=True
    )
    got = all_to_all(sent)
    pairs = call(
        read_keyval_kernel,
        ((2 * count, 128),) * 4,
        tokens,
        read_keyval,
        qk_gain,
        scratch=blocks(2 * count),
    )
    partial = call(read_kernel, ((devices, rows + 8, 128),), got, *swapped(pairs))
    own_rows, sent, *queries = call(
        self_project_kernel,
        ((rows, 1024), (devices, 2 * rows, 128)) + ((rows, 128),) * 4,
        all_to_all(partial),
        latents,
        read_out,
        self_qkv,
        qk_gain,
        scratch=blocks(rows),
    )
    attended = call(attend_kernel, ((rows, 128),) * 4, all_to_all(sent), *swapped(queries))
    latents_out, sent = call(
        write_project_kernel,
        ((rows, 1024), (devices, 2 * rows, 128)),
        *swapped(attended),
        own_rows,
        self_out,
        write_keyval,
        qk_gain,
        scratch=blocks(rows),
    )
    got = all_to_all(sent)
    queries = call(
        write_query_kernel,
        ((count, 128),) * 4,
        tokens,
        write_query,
        qk_gain,
        scratch=blocks(count),
    )
    q0, q1, q2, q3 = swapped(queries)
    a3, a2 = call(attend_kernel, ((count, 128),) * 2, got, q3, q2)
    a3, a2 = to_peer(a3, 3), to_peer(a2, 2)
    a1 = to_peer(call(attend_kernel, ((count, 128),), got, q1), 1)
    a0 = call(attend_kernel, ((count, 128),), got, q0)
    tokens_out = call(
        finish_kernel,
        ((count, 1024),),
        a0,
        a1,
        a2,
        a3,
        tokens,
        write_out,
        scratch=blocks(count),
    )
    return (tokens_out, latents_out)


def solution(mesh):
    torus = Mesh(mesh.devices.reshape(mesh.shape["ba"], 4, 4, 2), ("ba", "aa_0", "aa_1", "aa_2"))
    in_specs = (P(BA_AA, None), P(BA_AA, None), P(), P(), P(), P(), P(), P(), P(), P(), P())
    out_specs = (P(BA_AA, None), P(BA_AA, None))
    return jax.shard_map(
        per_device, mesh=torus, in_specs=in_specs, out_specs=out_specs, check_vma=False
    )
```

```python
import math

import jax
import jax.numpy as jnp
from jax import lax
from jax.experimental import pallas as pl
from jax.experimental.pallas import tpu as pltpu
from jax.sharding import Mesh
from jax.sharding import PartitionSpec as P

AA = ("aa_0", "aa_1", "aa_2")
BA_AA = ("ba", "aa_0", "aa_1", "aa_2")
HEADS = 8
PAIRS = 4
EPSILON = 1e-06
QUERY_SCALE = math.log2(math.e) / 8.0
F32, BF16 = jnp.float32, jnp.bfloat16


def own_pair():
    return 2 * lax.rem(lax.axis_index("aa_1"), 2) + lax.axis_index("aa_2")


def to_peer(x, k):
    swaps = [(i, i ^ k) for i in range(8)]
    return lax.ppermute(x, ("aa_1", "aa_2"), swaps)


def low_lanes(shape):
    return lax.broadcasted_iota(jnp.int32, shape, len(shape) - 1) < 64


def rms_rows(x):
    return (x * lax.rsqrt(jnp.mean(x * x, axis=-1, keepdims=True) + EPSILON)).astype(BF16)


def matmul(a, b):
    return jnp.dot(a, b, preferred_element_type=F32)


def matmul_t(a, b):
    return lax.dot_general(a, b, (((1,), (1,)), ((), ())), preferred_element_type=F32)


def head_norm(x, gain):
    row = lax.broadcasted_iota(jnp.int32, (256, 256), 0) // 64
    col = lax.broadcasted_iota(jnp.int32, (256, 256), 1) // 64
    averager = jnp.where(row == col, 1.0 / 64, 0.0).astype(BF16)
    squares = (x * x).astype(BF16)
    means = [matmul(squares[:, at : at + 256], averager) for at in range(0, x.shape[1], 256)]
    return x * lax.rsqrt(jnp.concatenate(means, axis=1) + EPSILON) * gain


def pair_of(x, p):
    return x[:, 128 * p : 128 * (p + 1)]


def attend(q, k, v):
    low = low_lanes(q.shape)
    values_low = low_lanes(v.shape)
    zero, one = jnp.zeros_like(q), jnp.ones_like(v)
    even = jnp.exp2(matmul_t(jnp.where(low, q, zero), k)).astype(BF16)
    odd = jnp.exp2(matmul_t(jnp.where(low, zero, q), k)).astype(BF16)
    even = matmul(even, jnp.where(values_low, v, one))
    odd = matmul(odd, jnp.where(values_low, one, v))
    return jnp.where(low, even, odd), jnp.where(low, odd, even)


def attend_whole(q, k, v):
    numerator, crossed = attend(q, k, v)
    return (numerator / pltpu.roll(crossed, 64, axis=1)).astype(BF16)


def hand_out(blocks_ref, outs):
    mine = own_pair()
    for k, out in enumerate(outs):
        out[...] = blocks_ref[mine ^ k]


def swap(x):
    return pltpu.roll(x, 64, axis=1)


def key_value_heads(keys, values):
    out = []
    for p in range(PAIRS):
        k, v = pair_of(keys, p), pair_of(values, p)
        low = low_lanes(k.shape)
        out.append(jnp.where(low, k, swap(v)).astype(BF16))
        out.append(jnp.where(low, swap(k), v).astype(BF16))
    return out


def query_heads(queries):
    half = queries.shape[0] // 2
    out = []
    for p in range(PAIRS):
        q = pair_of(queries, p)
        s = swap(q)
        low = low_lanes((half, 128))
        out.append(jnp.where(low, q[:half], s[half:]).astype(BF16))
        out.append(jnp.where(low, s[:half], q[half:]).astype(BF16))
    return out


def with_ones(kv, low):
    return jnp.where(low, jnp.ones_like(kv), kv)


def project_kernel(
    tokens_hbm,
    latents_hbm,
    wq_hbm,
    wkv_hbm,
    gain_hbm,
    send_ref,
    tokens_ref,
    latents_ref,
    wq_ref,
    wkv_ref,
    gain_ref,
    sems,
):
    half = wkv_ref.shape[1] // 2
    copies = [
        pltpu.make_async_copy(src, dst, sems.at[i])
        for i, (src, dst) in enumerate(
            (
                (gain_hbm, gain_ref),
                (latents_hbm, latents_ref),
                (tokens_hbm, tokens_ref),
                (wq_hbm, wq_ref),
                (wkv_hbm.at[:, :half], wkv_ref.at[:, :half]),
                (wkv_hbm.at[:, half:], wkv_ref.at[:, half:]),
            )
        )
    ]
    for copy in copies:
        copy.start()
    groups = send_ref.shape[0] // HEADS
    count = tokens_ref.shape[0] // groups
    copies[0].wait()
    copies[1].wait()
    latents = rms_rows(latents_ref[...].astype(F32))
    copies[2].wait()
    normed = rms_rows(tokens_ref[...].astype(F32))
    copies[3].wait()
    queries = head_norm(matmul(latents, wq_ref[...]), gain_ref[0:1, :] * QUERY_SCALE)
    for h, block in enumerate(query_heads(queries)):
        for g in range(groups):
            send_ref[g * HEADS + h, count:, :] = block
    copies[4].wait()
    keys = head_norm(matmul(normed, wkv_ref[:, :half]), gain_ref[1:2, :])
    copies[5].wait()
    values = matmul(normed, wkv_ref[:, half:])
    for h, block in enumerate(key_value_heads(keys, values)):
        for g in range(groups):
            send_ref[g * HEADS + h, :count, :] = block[g * count : (g + 1) * count]


def write_query_kernel(tokens_ref, wwq_ref, gain_ref, o0, o1, o2, o3, blocks_ref):
    normed = rms_rows(tokens_ref[...].astype(F32))
    queries = head_norm(matmul(normed, wwq_ref[...]), gain_ref[4:5, :] * QUERY_SCALE).astype(BF16)
    for p in range(PAIRS):
        blocks_ref[p] = pair_of(queries, p)
    hand_out(blocks_ref, (o0, o1, o2, o3))


def read_kernel(got_ref, out_ref):
    devices, rows, _ = got_ref.shape
    count = rows - 16
    kv = got_ref[:, :count, :].reshape(devices * count, 128)
    kv1 = with_ones(kv, low_lanes(kv.shape))
    step = 16
    for at in range(0, devices, step):
        packed = got_ref[at : at + step, count:, :].reshape(step * 16, 128).astype(F32)
        low = low_lanes(packed.shape)
        for half, q in enumerate((packed, swap(packed))):
            q = jnp.where(low, q, 0.0).astype(BF16)
            weights = jnp.exp2(matmul_t(q, kv)).astype(BF16)
            o = matmul(weights, kv1)
            out_ref[at : at + step, half * 16 : half * 16 + 16, :] = o.astype(BF16).reshape(
                step, 16, 128
            )


def self_project_kernel(
    got_ref, latents_ref, wo_ref, wqkv_ref, gain_ref, rows_ref, send_ref, q0, q1, q2, q3, blocks_ref
):
    devices = got_ref.shape[0]
    count = latents_ref.shape[0]
    attended = []
    for p in range(PAIRS):
        both = []
        for h in (2 * p, 2 * p + 1):
            total = got_ref[h].astype(F32)
            for g in range(1, devices // HEADS):
                total = total + got_ref[g * HEADS + h].astype(F32)
            both.append(total / swap(total))
        attended.append(jnp.where(low_lanes(both[0].shape), swap(both[0]), both[1]).astype(BF16))
    attended = jnp.concatenate(attended, axis=1)
    rows = (latents_ref[...].astype(F32) + matmul(attended, wo_ref[...])).astype(BF16)
    rows_ref[...] = rows
    triple = matmul(rms_rows(rows.astype(F32)), wqkv_ref[...])
    queries = head_norm(triple[:, :512], gain_ref[2:3, :] * QUERY_SCALE).astype(BF16)
    keys = head_norm(triple[:, 512:1024], gain_ref[3:4, :]).astype(BF16)
    values = triple[:, 1024:].astype(BF16)
    for p in range(PAIRS):
        blocks_ref[p] = pair_of(queries, p)
    for d in range(devices):
        send_ref[d, :count] = pair_of(keys, d % PAIRS)
        send_ref[d, count:] = pair_of(values, d % PAIRS)
    hand_out(blocks_ref, (q0, q1, q2, q3))


def keys_of(got_ref):
    devices, rows, _ = got_ref.shape
    return got_ref[:, : rows // 2].reshape(devices * rows // 2, 128)


def values_of(got_ref):
    devices, rows, _ = got_ref.shape
    return got_ref[:, rows // 2 :].reshape(devices * rows // 2, 128)


def attend_kernel(got_ref, *refs):
    queries, outs = refs[: len(refs) // 2], refs[len(refs) // 2 :]
    count = queries[0].shape[0]
    q = jnp.concatenate([q[...] for q in queries], axis=0)
    result = attend_whole(q, keys_of(got_ref), values_of(got_ref))
    for i, out in enumerate(outs):
        out[...] = result[i * count : (i + 1) * count]


def gathered(blocks_ref, parts):
    mine = own_pair()
    for k, part in enumerate(parts):
        blocks_ref[mine ^ k] = part[...]
    return jnp.concatenate([blocks_ref[p] for p in range(PAIRS)], axis=1)


def write_project_kernel(
    a0, a1, a2, a3, rows_ref, wo_ref, wkv_ref, gain_ref, latents_ref, send_ref, blocks_ref
):
    attended = gathered(blocks_ref, (a0, a1, a2, a3))
    rows = (rows_ref[...].astype(F32) + matmul(attended, wo_ref[...])).astype(BF16)
    latents_ref[...] = rows
    count = rows.shape[0]
    kv = matmul(rms_rows(rows.astype(F32)), wkv_ref[...])
    keys = head_norm(kv[:, :512], gain_ref[5:6, :]).astype(BF16)
    values = kv[:, 512:].astype(BF16)
    for d in range(send_ref.shape[0]):
        send_ref[d, :count] = pair_of(keys, d % PAIRS)
        send_ref[d, count:] = pair_of(values, d % PAIRS)


def finish_kernel(a0, a1, a2, a3, tokens_ref, wo_ref, out_ref, blocks_ref):
    update = matmul(gathered(blocks_ref, (a0, a1, a2, a3)), wo_ref[...])
    out_ref[...] = (tokens_ref[...].astype(F32) + update).astype(BF16)


def call(body, outs, *args, scratch=(), fetch=None):
    space = pltpu.HBM if fetch else pltpu.VMEM
    scratch = list(scratch)
    if fetch:
        scratch += [pltpu.VMEM(a.shape, a.dtype) for a in args]
        scratch.append(pltpu.SemaphoreType.DMA((len(args) + fetch,)))
        args = [pltpu.with_memory_space_constraint(a, space) for a in args]
    results = pl.pallas_call(
        body,
        out_shape=tuple(jax.ShapeDtypeStruct(s, BF16) for s in outs),
        in_specs=[pl.BlockSpec(memory_space=space)] * len(args),
        out_specs=tuple(pl.BlockSpec(memory_space=pltpu.VMEM) for _ in outs),
        scratch_shapes=scratch,
        compiler_params=pltpu.CompilerParams(vmem_limit_bytes=48 * 1024 * 1024),
        cost_estimate=pl.CostEstimate(
            flops=10**9,
            transcendentals=0,
            bytes_accessed=sum(a.size * a.dtype.itemsize for a in args),
        ),
    )(*args)
    return results if len(outs) > 1 else results[0]


def blocks(rows):
    return [pltpu.VMEM((PAIRS, rows, 128), BF16)]


def all_to_all(x):
    return lax.all_to_all(x, AA, split_axis=0, concat_axis=0, tiled=True)


def swapped(parts):
    there = {k: to_peer(parts[k], k) for k in (3, 2, 1)}
    return (parts[0], there[1], there[2], there[3])


def per_device(
    tokens,
    latents,
    read_query,
    read_keyval,
    read_out,
    self_qkv,
    self_out,
    write_query,
    write_keyval,
    write_out,
    qk_gain,
):
    count, rows = tokens.shape[0], latents.shape[0]
    devices = lax.axis_size(AA)
    sent = call(
        project_kernel,
        ((devices, count * HEADS // devices + 16, 128),),
        tokens,
        latents,
        read_query,
        read_keyval,
        qk_gain,
        fetch=1,
    )
    partial = call(read_kernel, ((devices, rows, 128),), all_to_all(sent))
    own_rows, sent, *queries = call(
        self_project_kernel,
        ((rows, 1024), (devices, 2 * rows, 128)) + ((rows, 128),) * 4,
        all_to_all(partial),
        latents,
        read_out,
        self_qkv,
        qk_gain,
        scratch=blocks(rows),
    )
    asked = call(
        write_query_kernel,
        ((count, 128),) * 4,
        tokens,
        write_query,
        qk_gain,
        scratch=blocks(count),
    )
    got, asked = lax.optimization_barrier((all_to_all(sent), asked))
    attended = call(attend_kernel, ((rows, 128),) * 4, got, *swapped(queries))
    latents_out, sent = call(
        write_project_kernel,
        ((rows, 1024), (devices, 2 * rows, 128)),
        *swapped(attended),
        own_rows,
        self_out,
        write_keyval,
        qk_gain,
        scratch=blocks(rows),
    )
    got = all_to_all(sent)
    q0, q1, q2, q3 = swapped(asked)
    a3, a2 = call(attend_kernel, ((count, 128),) * 2, got, q3, q2)
    a3, a2 = to_peer(a3, 3), to_peer(a2, 2)
    a1 = to_peer(call(attend_kernel, ((count, 128),), got, q1), 1)
    a0 = call(attend_kernel, ((count, 128),), got, q0)
    tokens_out = call(
        finish_kernel,
        ((count, 1024),),
        a0,
        a1,
        a2,
        a3,
        tokens,
        write_out,
        scratch=blocks(count),
    )
    return (tokens_out, latents_out)


def solution(mesh):
    torus = Mesh(mesh.devices.reshape(mesh.shape["ba"], 4, 4, 2), ("ba", "aa_0", "aa_1", "aa_2"))
    in_specs = (P(BA_AA, None), P(BA_AA, None), P(), P(), P(), P(), P(), P(), P(), P(), P())
    out_specs = (P(BA_AA, None), P(BA_AA, None))
    return jax.shard_map(
        per_device, mesh=torus, in_specs=in_specs, out_specs=out_specs, check_vma=False
    )
```

```python
import math

import jax
import jax.numpy as jnp
from jax import lax
from jax.experimental import pallas as pl
from jax.experimental.pallas import tpu as pltpu
from jax.sharding import Mesh
from jax.sharding import PartitionSpec as P

AA = ("aa_0", "aa_1", "aa_2")
BA_AA = ("ba", "aa_0", "aa_1", "aa_2")
HEADS = 8
PAIRS = 4
EPSILON = 1e-06
QUERY_SCALE = math.log2(math.e) / 8.0
F32, BF16 = jnp.float32, jnp.bfloat16


def own_pair():
    return 2 * lax.rem(lax.axis_index("aa_1"), 2) + lax.axis_index("aa_2")


def to_peer(x, k):
    swaps = [(i, i ^ k) for i in range(8)]
    return lax.ppermute(x, ("aa_1", "aa_2"), swaps)


def low_lanes(shape):
    return lax.broadcasted_iota(jnp.int32, shape, len(shape) - 1) < 64


def rms_rows(x):
    return (x * lax.rsqrt(jnp.mean(x * x, axis=-1, keepdims=True) + EPSILON)).astype(BF16)


def matmul(a, b):
    return jnp.dot(a, b, preferred_element_type=F32)


def matmul_t(a, b):
    return lax.dot_general(a, b, (((1,), (1,)), ((), ())), preferred_element_type=F32)


def head_norm(x, gain):
    row = lax.broadcasted_iota(jnp.int32, (256, 256), 0) // 64
    col = lax.broadcasted_iota(jnp.int32, (256, 256), 1) // 64
    averager = jnp.where(row == col, 1.0 / 64, 0.0).astype(BF16)
    squares = (x * x).astype(BF16)
    means = [matmul(squares[:, at : at + 256], averager) for at in range(0, x.shape[1], 256)]
    return x * lax.rsqrt(jnp.concatenate(means, axis=1) + EPSILON) * gain


def pair_of(x, p):
    return x[:, 128 * p : 128 * (p + 1)]


def attend(q, k, v):
    low = low_lanes(q.shape)
    values_low = low_lanes(v.shape)
    zero, one = jnp.zeros_like(q), jnp.ones_like(v)
    even = jnp.exp2(matmul_t(jnp.where(low, q, zero), k)).astype(BF16)
    odd = jnp.exp2(matmul_t(jnp.where(low, zero, q), k)).astype(BF16)
    even = matmul(even, jnp.where(values_low, v, one))
    odd = matmul(odd, jnp.where(values_low, one, v))
    return jnp.where(low, even, odd), jnp.where(low, odd, even)


def attend_whole(q, k, v):
    numerator, crossed = attend(q, k, v)
    return (numerator / pltpu.roll(crossed, 64, axis=1)).astype(BF16)


def hand_out(blocks_ref, outs):
    mine = own_pair()
    for k, out in enumerate(outs):
        out[...] = blocks_ref[mine ^ k]


def swap(x):
    return pltpu.roll(x, 64, axis=1)


def key_value_heads(keys, values):
    out = []
    for p in range(PAIRS):
        k, v = pair_of(keys, p), pair_of(values, p)
        low = low_lanes(k.shape)
        out.append(jnp.where(low, k, swap(v)).astype(BF16))
        out.append(jnp.where(low, swap(k), v).astype(BF16))
    return out


def query_heads(queries):
    half = queries.shape[0] // 2
    out = []
    for p in range(PAIRS):
        q = pair_of(queries, p)
        s = swap(q)
        low = low_lanes((half, 128))
        out.append(jnp.where(low, q[:half], s[half:]).astype(BF16))
        out.append(jnp.where(low, s[:half], q[half:]).astype(BF16))
    return out


def with_ones(kv, low):
    return jnp.where(low, jnp.ones_like(kv), kv)


def project_kernel(
    tokens_hbm,
    latents_hbm,
    wq_hbm,
    wkv_hbm,
    gain_hbm,
    send_ref,
    tokens_ref,
    latents_ref,
    wq_ref,
    wkv_ref,
    gain_ref,
    sems,
):
    half = wkv_ref.shape[1] // 2
    copies = [
        pltpu.make_async_copy(src, dst, sems.at[i])
        for i, (src, dst) in enumerate(
            (
                (gain_hbm, gain_ref),
                (latents_hbm, latents_ref),
                (tokens_hbm, tokens_ref),
                (wq_hbm, wq_ref),
                (wkv_hbm.at[:, :half], wkv_ref.at[:, :half]),
                (wkv_hbm.at[:, half:], wkv_ref.at[:, half:]),
            )
        )
    ]
    for copy in copies:
        copy.start()
    groups = send_ref.shape[0] // HEADS
    count = tokens_ref.shape[0] // groups
    copies[0].wait()
    copies[1].wait()
    latents = rms_rows(latents_ref[...].astype(F32))
    copies[2].wait()
    normed = rms_rows(tokens_ref[...].astype(F32))
    copies[3].wait()
    queries = head_norm(matmul(latents, wq_ref[...]), gain_ref[0:1, :] * QUERY_SCALE)
    for h, block in enumerate(query_heads(queries)):
        for g in range(groups):
            send_ref[g * HEADS + h, count:, :] = block
    copies[4].wait()
    keys = head_norm(matmul(normed, wkv_ref[:, :half]), gain_ref[1:2, :])
    copies[5].wait()
    values = matmul(normed, wkv_ref[:, half:])
    for h, block in enumerate(key_value_heads(keys, values)):
        for g in range(groups):
            send_ref[g * HEADS + h, :count, :] = block[g * count : (g + 1) * count]


def write_query_kernel(tokens_ref, wwq_ref, gain_ref, o0, o1, o2, o3, blocks_ref):
    normed = rms_rows(tokens_ref[...].astype(F32))
    queries = head_norm(matmul(normed, wwq_ref[...]), gain_ref[4:5, :] * QUERY_SCALE).astype(BF16)
    for p in range(PAIRS):
        blocks_ref[p] = pair_of(queries, p)
    hand_out(blocks_ref, (o0, o1, o2, o3))


def read_kernel(got_ref, out_ref):
    devices, rows, _ = got_ref.shape
    count = rows - 16
    kv = got_ref[:, :count, :].reshape(devices * count, 128)
    kv1 = with_ones(kv, low_lanes(kv.shape))
    step = 8
    for at in range(0, devices, step):
        packed = got_ref[at : at + step, count:, :].reshape(step * 16, 128).astype(F32)
        low = low_lanes(packed.shape)
        q = jnp.concatenate([packed, swap(packed)], axis=0)
        q = jnp.where(low_lanes(q.shape), q, 0.0).astype(BF16)
        o = matmul(jnp.exp2(matmul_t(q, kv)).astype(BF16), kv1)
        top, bottom = o[: step * 16], o[step * 16 :]
        numerators = jnp.where(low, swap(top), bottom)
        out_ref[at : at + step, :16] = numerators.astype(BF16).reshape(step, 16, 128)
        denominators = jnp.where(low, top, swap(bottom)).reshape(step, 2, 8, 128)
        part = lax.broadcasted_iota(jnp.int32, (step, 8, 128), 2) // 32 % 2
        denominators = jnp.where(part == 0, denominators[:, 0], denominators[:, 1])
        out_ref[at : at + step, 16:] = denominators.astype(BF16)


def unpacked_heads(got_ref):
    groups = got_ref.shape[0] // HEADS
    first = lax.broadcasted_iota(jnp.int32, (8, 128), 1) // 32 % 2 == 0
    heads = []
    for h in range(HEADS):
        total = got_ref[h].astype(F32)
        for g in range(1, groups):
            total = total + got_ref[g * HEADS + h].astype(F32)
        numerators, packed = total[:16], total[16:]
        top, bottom = jnp.where(first, packed, 0.0), jnp.where(first, 0.0, packed)
        top = top + pltpu.roll(top, 32, axis=1)
        bottom = bottom + pltpu.roll(bottom, 96, axis=1)
        heads.append(numerators / jnp.concatenate([top, bottom], axis=0))
    return heads


def self_project_kernel(
    got_ref, latents_ref, wo_ref, wqkv_ref, gain_ref, rows_ref, send_ref, q0, q1, q2, q3, blocks_ref
):
    devices = got_ref.shape[0]
    count = latents_ref.shape[0]
    attended = []
    heads = unpacked_heads(got_ref)
    low = low_lanes(heads[0].shape)
    for e, o in zip(heads[0::2], heads[1::2]):
        top, bottom = jnp.where(low, e, swap(o)), jnp.where(low, swap(e), o)
        attended.append(jnp.concatenate([top, bottom], axis=0).astype(BF16))
    attended = jnp.concatenate(attended, axis=1)
    rows = (latents_ref[...].astype(F32) + matmul(attended, wo_ref[...])).astype(BF16)
    rows_ref[...] = rows
    triple = matmul(rms_rows(rows.astype(F32)), wqkv_ref[...])
    queries = head_norm(triple[:, :512], gain_ref[2:3, :] * QUERY_SCALE).astype(BF16)
    keys = head_norm(triple[:, 512:1024], gain_ref[3:4, :]).astype(BF16)
    values = triple[:, 1024:].astype(BF16)
    for p in range(PAIRS):
        blocks_ref[p] = pair_of(queries, p)
    for d in range(devices):
        send_ref[d, :count] = pair_of(keys, d % PAIRS)
        send_ref[d, count:] = pair_of(values, d % PAIRS)
    hand_out(blocks_ref, (q0, q1, q2, q3))


def keys_of(got_ref):
    devices, rows, _ = got_ref.shape
    return got_ref[:, : rows // 2].reshape(devices * rows // 2, 128)


def values_of(got_ref):
    devices, rows, _ = got_ref.shape
    return got_ref[:, rows // 2 :].reshape(devices * rows // 2, 128)


def attend_kernel(got_ref, *refs):
    queries, outs = refs[: len(refs) // 2], refs[len(refs) // 2 :]
    count = queries[0].shape[0]
    q = jnp.concatenate([q[...] for q in queries], axis=0)
    result = attend_whole(q, keys_of(got_ref), values_of(got_ref))
    for i, out in enumerate(outs):
        out[...] = result[i * count : (i + 1) * count]


def gathered(blocks_ref, parts):
    mine = own_pair()
    for k, part in enumerate(parts):
        blocks_ref[mine ^ k] = part[...]
    return jnp.concatenate([blocks_ref[p] for p in range(PAIRS)], axis=1)


def write_project_kernel(
    a3, a2, a1, a0, rows_ref, wo_ref, wkv_ref, gain_ref, latents_ref, send_ref, blocks_ref
):
    attended = gathered(blocks_ref, (a0, a1, a2, a3))
    rows = (rows_ref[...].astype(F32) + matmul(attended, wo_ref[...])).astype(BF16)
    latents_ref[...] = rows
    count = rows.shape[0]
    kv = matmul(rms_rows(rows.astype(F32)), wkv_ref[...])
    keys = head_norm(kv[:, :512], gain_ref[5:6, :]).astype(BF16)
    values = kv[:, 512:].astype(BF16)
    for d in range(send_ref.shape[0]):
        send_ref[d, :count] = pair_of(keys, d % PAIRS)
        send_ref[d, count:] = pair_of(values, d % PAIRS)


def finish_kernel(a0, a1, a2, a3, tokens_ref, wo_ref, out_ref, blocks_ref):
    update = matmul(gathered(blocks_ref, (a0, a1, a2, a3)), wo_ref[...])
    out_ref[...] = (tokens_ref[...].astype(F32) + update).astype(BF16)


def call(body, outs, *args, scratch=(), fetch=None):
    space = pltpu.HBM if fetch else pltpu.VMEM
    scratch = list(scratch)
    if fetch:
        scratch += [pltpu.VMEM(a.shape, a.dtype) for a in args]
        scratch.append(pltpu.SemaphoreType.DMA((len(args) + fetch,)))
        args = [pltpu.with_memory_space_constraint(a, space) for a in args]
    results = pl.pallas_call(
        body,
        out_shape=tuple(jax.ShapeDtypeStruct(s, BF16) for s in outs),
        in_specs=[pl.BlockSpec(memory_space=space)] * len(args),
        out_specs=tuple(pl.BlockSpec(memory_space=pltpu.VMEM) for _ in outs),
        scratch_shapes=scratch,
        compiler_params=pltpu.CompilerParams(vmem_limit_bytes=48 * 1024 * 1024),
        cost_estimate=pl.CostEstimate(
            flops=10**9,
            transcendentals=0,
            bytes_accessed=sum(a.size * a.dtype.itemsize for a in args),
        ),
    )(*args)
    return results if len(outs) > 1 else results[0]


def blocks(rows):
    return [pltpu.VMEM((PAIRS, rows, 128), BF16)]


def all_to_all(x):
    return lax.all_to_all(x, AA, split_axis=0, concat_axis=0, tiled=True)


def swapped(parts):
    return tuple(to_peer(parts[k], k) for k in (3, 2, 1)) + (parts[0],)


def per_device(
    tokens,
    latents,
    read_query,
    read_keyval,
    read_out,
    self_qkv,
    self_out,
    write_query,
    write_keyval,
    write_out,
    qk_gain,
):
    count, rows = tokens.shape[0], latents.shape[0]
    devices = lax.axis_size(AA)
    sent = call(
        project_kernel,
        ((devices, count * HEADS // devices + 16, 128),),
        tokens,
        latents,
        read_query,
        read_keyval,
        qk_gain,
        fetch=1,
    )
    partial = call(read_kernel, ((devices, 24, 128),), all_to_all(sent))
    own_rows, sent, *queries = call(
        self_project_kernel,
        ((rows, 1024), (devices, 2 * rows, 128)) + ((rows, 128),) * 4,
        all_to_all(partial),
        latents,
        read_out,
        self_qkv,
        qk_gain,
        scratch=blocks(rows),
    )
    asked = call(
        write_query_kernel,
        ((count, 128),) * 4,
        tokens,
        write_query,
        qk_gain,
        scratch=blocks(count),
    )
    got, asked = lax.optimization_barrier((all_to_all(sent), asked))
    attended = call(attend_kernel, ((rows, 128),) * 4, got, *swapped(queries))[::-1]
    latents_out, sent = call(
        write_project_kernel,
        ((rows, 1024), (devices, 2 * rows, 128)),
        *swapped(attended),
        own_rows,
        self_out,
        write_keyval,
        qk_gain,
        scratch=blocks(rows),
    )
    got = all_to_all(sent)
    q3, q2, q1, q0 = swapped(asked)
    a3, a2 = call(attend_kernel, ((count, 128),) * 2, got, q3, q2)
    a3, a2 = to_peer(a3, 3), to_peer(a2, 2)
    a1 = to_peer(call(attend_kernel, ((count, 128),), got, q1), 1)
    a0 = call(attend_kernel, ((count, 128),), got, q0)
    tokens_out = call(
        finish_kernel,
        ((count, 1024),),
        a0,
        a1,
        a2,
        a3,
        tokens,
        write_out,
        scratch=blocks(count),
    )
    return (tokens_out, latents_out)


def solution(mesh):
    torus = Mesh(mesh.devices.reshape(mesh.shape["ba"], 4, 4, 2), ("ba", "aa_0", "aa_1", "aa_2"))
    in_specs = (P(BA_AA, None), P(BA_AA, None), P(), P(), P(), P(), P(), P(), P(), P(), P())
    out_specs = (P(BA_AA, None), P(BA_AA, None))
    return jax.shard_map(
        per_device, mesh=torus, in_specs=in_specs, out_specs=out_specs, check_vma=False
    )
```

```python
import math

import jax
import jax.numpy as jnp
from jax import lax
from jax.experimental import pallas as pl
from jax.experimental.pallas import tpu as pltpu
from jax.sharding import Mesh
from jax.sharding import PartitionSpec as P


AA = ("aa_0", "aa_1", "aa_2")
BA_AA = ("ba", "aa_0", "aa_1", "aa_2")
HEADS = 8
PAIRS = 4
EPSILON = 1e-06
QUERY_SCALE = math.log2(math.e) / 8.0
F32, BF16 = jnp.float32, jnp.bfloat16


def own_pair():
    return 2 * lax.rem(lax.axis_index("aa_1"), 2) + lax.axis_index("aa_2")


def to_peer(x, k):
    swaps = [(i, i ^ k) for i in range(8)]
    return lax.ppermute(x, ("aa_1", "aa_2"), swaps)


def low_lanes(shape):
    return lax.broadcasted_iota(jnp.int32, shape, len(shape) - 1) < 64


def rms_rows(x):
    return (x * lax.rsqrt(jnp.mean(x * x, axis=-1, keepdims=True) + EPSILON)).astype(BF16)


def matmul(a, b):
    return jnp.dot(a, b, preferred_element_type=F32)


def matmul_t(a, b):
    return lax.dot_general(a, b, (((1,), (1,)), ((), ())), preferred_element_type=F32)


def head_norm(x, gain):
    row = lax.broadcasted_iota(jnp.int32, (256, 256), 0) // 64
    col = lax.broadcasted_iota(jnp.int32, (256, 256), 1) // 64
    averager = jnp.where(row == col, 1.0 / 64, 0.0).astype(BF16)
    squares = (x * x).astype(BF16)
    means = [matmul(squares[:, at : at + 256], averager) for at in range(0, x.shape[1], 256)]
    return x * lax.rsqrt(jnp.concatenate(means, axis=1) + EPSILON) * gain


def pair_of(x, p):
    return x[:, 128 * p : 128 * (p + 1)]


def attend(q, k, v):
    low = low_lanes(q.shape)
    values_low = low_lanes(v.shape)
    zero, one = jnp.zeros_like(q), jnp.ones_like(v)
    even = jnp.exp2(matmul_t(jnp.where(low, q, zero), k)).astype(BF16)
    odd = jnp.exp2(matmul_t(jnp.where(low, zero, q), k)).astype(BF16)
    even = matmul(even, jnp.where(values_low, v, one))
    odd = matmul(odd, jnp.where(values_low, one, v))
    return jnp.where(low, even, odd), jnp.where(low, odd, even)


def attend_whole(q, k, v):
    numerator, crossed = attend(q, k, v)
    return (numerator / pltpu.roll(crossed, 64, axis=1)).astype(BF16)


def hand_out(blocks_ref, outs):
    mine = own_pair()
    for k, out in enumerate(outs):
        out[...] = blocks_ref[mine ^ k]


def swap(x):
    return pltpu.roll(x, 64, axis=1)


def key_value_heads(keys, values):
    out = []
    for p in range(PAIRS):
        k, v = pair_of(keys, p), pair_of(values, p)
        low = low_lanes(k.shape)
        out.append(jnp.where(low, k, swap(v)).astype(BF16))
        out.append(jnp.where(low, swap(k), v).astype(BF16))
    return out


def query_heads(queries):
    half = queries.shape[0] // 2
    out = []
    for p in range(PAIRS):
        q = pair_of(queries, p)
        s = swap(q)
        low = low_lanes((half, 128))
        out.append(jnp.where(low, q[:half], s[half:]).astype(BF16))
        out.append(jnp.where(low, s[:half], q[half:]).astype(BF16))
    return out


def with_ones(kv, low):
    return jnp.where(low, jnp.ones_like(kv), kv)


def project_kernel(
    tokens_hbm,
    latents_hbm,
    wq_hbm,
    wkv_hbm,
    gain_hbm,
    send_ref,
    tokens_ref,
    latents_ref,
    wq_ref,
    wkv_ref,
    gain_ref,
    sems,
):
    half = wkv_ref.shape[1] // 2
    copies = [
        pltpu.make_async_copy(src, dst, sems.at[i])
        for i, (src, dst) in enumerate(
            (
                (gain_hbm, gain_ref),
                (latents_hbm, latents_ref),
                (tokens_hbm, tokens_ref),
                (wq_hbm, wq_ref),
                (wkv_hbm.at[:, :half], wkv_ref.at[:, :half]),
                (wkv_hbm.at[:, half:], wkv_ref.at[:, half:]),
            )
        )
    ]
    for copy in copies:
        copy.start()
    groups = send_ref.shape[0] // HEADS
    count = tokens_ref.shape[0] // groups
    copies[0].wait()
    copies[1].wait()
    latents = rms_rows(latents_ref[...].astype(F32))
    copies[2].wait()
    normed = rms_rows(tokens_ref[...].astype(F32))
    copies[3].wait()
    queries = head_norm(matmul(latents, wq_ref[...]), gain_ref[0:1, :] * QUERY_SCALE)
    for h, block in enumerate(query_heads(queries)):
        for g in range(groups):
            send_ref[g * HEADS + h, count:, :] = block
    copies[4].wait()
    keys = head_norm(matmul(normed, wkv_ref[:, :half]), gain_ref[1:2, :])
    copies[5].wait()
    values = matmul(normed, wkv_ref[:, half:])
    for h, block in enumerate(key_value_heads(keys, values)):
        for g in range(groups):
            send_ref[g * HEADS + h, :count, :] = block[g * count : (g + 1) * count]


def write_query_kernel(tokens_ref, wwq_ref, gain_ref, o0, o1, o2, o3, blocks_ref):
    normed = rms_rows(tokens_ref[...].astype(F32))
    queries = head_norm(matmul(normed, wwq_ref[...]), gain_ref[4:5, :] * QUERY_SCALE).astype(BF16)
    for p in range(PAIRS):
        blocks_ref[p] = pair_of(queries, p)
    hand_out(blocks_ref, (o0, o1, o2, o3))


def read_kernel(got_ref, out_ref):
    devices, rows, _ = got_ref.shape
    count = rows - 16
    kv = got_ref[:, :count, :].reshape(devices * count, 128)
    kv1 = with_ones(kv, low_lanes(kv.shape))
    step = 8
    for at in range(0, devices, step):
        packed = got_ref[at : at + step, count:, :].reshape(step * 16, 128).astype(F32)
        low = low_lanes(packed.shape)
        q = jnp.concatenate([packed, swap(packed)], axis=0)
        q = jnp.where(low_lanes(q.shape), q, 0.0).astype(BF16)
        o = matmul(jnp.exp2(matmul_t(q, kv)).astype(BF16), kv1)
        top, bottom = o[: step * 16], o[step * 16 :]
        numerators = jnp.where(low, swap(top), bottom)
        out_ref[at : at + step, :16] = numerators.astype(BF16).reshape(step, 16, 128)
        denominators = jnp.where(low, top, swap(bottom)).reshape(step, 2, 8, 128)
        part = lax.broadcasted_iota(jnp.int32, (step, 8, 128), 2) // 32 % 2
        denominators = jnp.where(part == 0, denominators[:, 0], denominators[:, 1])
        out_ref[at : at + step, 16:] = denominators.astype(BF16)


def unpacked_heads(got_ref):
    groups = got_ref.shape[0] // HEADS
    first = lax.broadcasted_iota(jnp.int32, (8, 128), 1) // 32 % 2 == 0
    heads = []
    for h in range(HEADS):
        total = got_ref[h].astype(F32)
        for g in range(1, groups):
            total = total + got_ref[g * HEADS + h].astype(F32)
        numerators, packed = total[:16], total[16:]
        top, bottom = jnp.where(first, packed, 0.0), jnp.where(first, 0.0, packed)
        top = top + pltpu.roll(top, 32, axis=1)
        bottom = bottom + pltpu.roll(bottom, 96, axis=1)
        heads.append(numerators / jnp.concatenate([top, bottom], axis=0))
    return heads


def to_each_quad(kv_ref, send_ref, sems):
    copies = [
        pltpu.make_async_copy(kv_ref, send_ref.at[pl.ds(PAIRS * g, PAIRS)], sems.at[g])
        for g in range(send_ref.shape[0] // PAIRS)
    ]
    for copy in copies:
        copy.start()
    return copies


def self_project_kernel(
    got_ref, latents_ref, wo_ref, wqkv_ref, gain_ref, rows_ref, send_ref, q0, q1, q2, q3, blocks_ref, kv_ref, sems
):
    count = latents_ref.shape[0]
    attended = []
    heads = unpacked_heads(got_ref)
    low = low_lanes(heads[0].shape)
    for e, o in zip(heads[0::2], heads[1::2]):
        top, bottom = jnp.where(low, e, swap(o)), jnp.where(low, swap(e), o)
        attended.append(jnp.concatenate([top, bottom], axis=0).astype(BF16))
    attended = jnp.concatenate(attended, axis=1)
    rows = (latents_ref[...].astype(F32) + matmul(attended, wo_ref[...])).astype(BF16)
    rows_ref[...] = rows
    normed = rms_rows(rows.astype(F32))
    pairs = matmul(normed, wqkv_ref[:, 512:])
    keys = head_norm(pairs[:, :512], gain_ref[3:4, :]).astype(BF16)
    values = pairs[:, 512:].astype(BF16)
    for p in range(PAIRS):
        kv_ref[p, :count] = pair_of(keys, p)
        kv_ref[p, count:] = pair_of(values, p)
    copies = to_each_quad(kv_ref, send_ref, sems)
    queries = matmul(normed, wqkv_ref[:, :512])
    queries = head_norm(queries, gain_ref[2:3, :] * QUERY_SCALE).astype(BF16)
    for p in range(PAIRS):
        blocks_ref[p] = pair_of(queries, p)
    hand_out(blocks_ref, (q0, q1, q2, q3))
    for copy in copies:
        copy.wait()


def keys_of(got_ref):
    devices, rows, _ = got_ref.shape
    return got_ref[:, : rows // 2].reshape(devices * rows // 2, 128)


def values_of(got_ref):
    devices, rows, _ = got_ref.shape
    return got_ref[:, rows // 2 :].reshape(devices * rows // 2, 128)


def attend_kernel(got_ref, *refs):
    queries, outs = refs[: len(refs) // 2], refs[len(refs) // 2 :]
    count = queries[0].shape[0]
    q = jnp.concatenate([q[...] for q in queries], axis=0)
    result = attend_whole(q, keys_of(got_ref), values_of(got_ref))
    for i, out in enumerate(outs):
        out[...] = result[i * count : (i + 1) * count]


def gathered(blocks_ref, parts):
    mine = own_pair()
    for k, part in enumerate(parts):
        blocks_ref[mine ^ k] = part[...]
    return jnp.concatenate([blocks_ref[p] for p in range(PAIRS)], axis=1)


def write_project_kernel(
    a3, a2, a1, a0, rows_ref, wo_ref, wkv_ref, gain_ref, latents_ref, send_ref, blocks_ref, kv_ref, sems
):
    attended = gathered(blocks_ref, (a0, a1, a2, a3))
    rows = (rows_ref[...].astype(F32) + matmul(attended, wo_ref[...])).astype(BF16)
    latents_ref[...] = rows
    count = rows.shape[0]
    kv = matmul(rms_rows(rows.astype(F32)), wkv_ref[...])
    keys = head_norm(kv[:, :512], gain_ref[5:6, :]).astype(BF16)
    values = kv[:, 512:].astype(BF16)
    for p in range(PAIRS):
        kv_ref[p, :count] = pair_of(keys, p)
        kv_ref[p, count:] = pair_of(values, p)
    for copy in to_each_quad(kv_ref, send_ref, sems):
        copy.wait()


def finish_kernel(a0, a1, a2, a3, tokens_ref, wo_ref, out_hbm, blocks_ref, out_ref, sems):
    attended = gathered(blocks_ref, (a0, a1, a2, a3))
    half = attended.shape[0] // 2
    copies = []
    for i in range(2):
        part = pl.ds(i * half, half)
        update = matmul(attended[i * half : (i + 1) * half], wo_ref[...])
        out_ref[part] = (tokens_ref[part].astype(F32) + update).astype(BF16)
        copies.append(pltpu.make_async_copy(out_ref.at[part], out_hbm.at[part], sems.at[i]))
        copies[-1].start()
    for copy in copies:
        copy.wait()


def call(body, outs, *args, scratch=(), fetch=None, kept=()):
    space = pltpu.HBM if fetch else pltpu.VMEM
    scratch = list(scratch)
    if fetch:
        scratch += [pltpu.VMEM(a.shape, a.dtype) for a in args]
        scratch.append(pltpu.SemaphoreType.DMA((len(args) + fetch,)))
        args = [pltpu.with_memory_space_constraint(a, space) for a in args]
    results = pl.pallas_call(
        body,
        out_shape=tuple(jax.ShapeDtypeStruct(s, BF16) for s in outs),
        in_specs=[pl.BlockSpec(memory_space=space)] * len(args),
        out_specs=tuple(
            pl.BlockSpec(memory_space=pltpu.HBM if i in kept else pltpu.VMEM)
            for i in range(len(outs))
        ),
        scratch_shapes=scratch,
        compiler_params=pltpu.CompilerParams(vmem_limit_bytes=48 * 1024 * 1024),
        cost_estimate=pl.CostEstimate(
            flops=10**9,
            transcendentals=0,
            bytes_accessed=sum(a.size * a.dtype.itemsize for a in args),
        ),
    )(*args)
    return results if len(outs) > 1 else results[0]


def blocks(rows):
    return [pltpu.VMEM((PAIRS, rows, 128), BF16)]


def staged(shape, count):
    return [pltpu.VMEM(shape, BF16), pltpu.SemaphoreType.DMA((count,))]


def all_to_all(x):
    return lax.all_to_all(x, AA, split_axis=0, concat_axis=0, tiled=True)


def swapped(parts):
    return tuple(to_peer(parts[k], k) for k in (3, 2, 1)) + (parts[0],)


def layer(
    tokens,
    latents,
    read_query,
    read_keyval,
    read_out,
    self_qkv,
    self_out,
    write_query,
    write_keyval,
    write_out,
    qk_gain,
):
    count, rows = tokens.shape[0], latents.shape[0]
    devices = lax.axis_size(AA)
    sent = call(
        project_kernel,
        ((devices, count * HEADS // devices + 16, 128),),
        tokens,
        latents,
        read_query,
        read_keyval,
        qk_gain,
        fetch=1,
    )
    partial = call(read_kernel, ((devices, 24, 128),), all_to_all(sent))
    own_rows, sent, *queries = call(
        self_project_kernel,
        ((rows, 1024), (devices, 2 * rows, 128)) + ((rows, 128),) * 4,
        all_to_all(partial),
        latents,
        read_out,
        self_qkv,
        qk_gain,
        scratch=blocks(rows) + staged((PAIRS, 2 * rows, 128), devices // PAIRS),
        kept=(1,),
    )
    asked = call(
        write_query_kernel,
        ((count, 128),) * 4,
        tokens,
        write_query,
        qk_gain,
        scratch=blocks(count),
    )
    q3, q2, q1, q0 = swapped(asked)
    got = all_to_all(sent)
    queries = swapped(queries)
    attended = call(attend_kernel, ((rows, 128),) * 4, got, *queries)[::-1]
    latents_out, sent = call(
        write_project_kernel,
        ((rows, 1024), (devices, 2 * rows, 128)),
        *swapped(attended),
        own_rows,
        self_out,
        write_keyval,
        qk_gain,
        scratch=blocks(rows) + staged((PAIRS, 2 * rows, 128), devices // PAIRS),
        kept=(1,),
    )
    got = all_to_all(sent)
    a3, a2 = call(attend_kernel, ((count, 128),) * 2, got, q3, q2)
    a3, a2 = to_peer(a3, 3), to_peer(a2, 2)
    a1 = to_peer(call(attend_kernel, ((count, 128),), got, q1), 1)
    a0 = call(attend_kernel, ((count, 128),), got, q0)
    tokens_out = call(
        finish_kernel,
        ((count, 1024),),
        a0,
        a1,
        a2,
        a3,
        tokens,
        write_out,
        scratch=blocks(count) + staged((count, 1024), 2),
        kept=(0,),
    )
    return (tokens_out, latents_out)


def solution(mesh):
    torus = Mesh(mesh.devices.reshape(mesh.shape["ba"], 4, 4, 2), ("ba", "aa_0", "aa_1", "aa_2"))
    in_specs = (P(BA_AA, None), P(BA_AA, None), P(), P(), P(), P(), P(), P(), P(), P(), P())
    out_specs = (P(BA_AA, None), P(BA_AA, None))
    return jax.shard_map(layer, mesh=torus, in_specs=in_specs, out_specs=out_specs, check_vma=False)
```

```python
import math

import jax
import jax.numpy as jnp
from jax import lax
from jax.experimental import pallas as pl
from jax.experimental.pallas import tpu as pltpu
from jax.sharding import Mesh
from jax.sharding import PartitionSpec as P


AA = ("aa_0", "aa_1", "aa_2")
BA_AA = ("ba", "aa_0", "aa_1", "aa_2")
HEADS = 8
PAIRS = 4
EPSILON = 1e-06
QUERY_SCALE = math.log2(math.e) / 8.0
F32, BF16 = jnp.float32, jnp.bfloat16


def own_pair():
    return 2 * lax.rem(lax.axis_index("aa_1"), 2) + lax.axis_index("aa_2")


def to_peer(x, k):
    swaps = [(i, i ^ k) for i in range(8)]
    return lax.ppermute(x, ("aa_1", "aa_2"), swaps)


def low_lanes(shape):
    return lax.broadcasted_iota(jnp.int32, shape, len(shape) - 1) < 64


def rms_rows(x):
    return (x * lax.rsqrt(jnp.mean(x * x, axis=-1, keepdims=True) + EPSILON)).astype(BF16)


def matmul(a, b):
    return jnp.dot(a, b, preferred_element_type=F32)


def matmul_t(a, b):
    return lax.dot_general(a, b, (((1,), (1,)), ((), ())), preferred_element_type=F32)


def head_norm(x, gain):
    row = lax.broadcasted_iota(jnp.int32, (256, 256), 0) // 64
    col = lax.broadcasted_iota(jnp.int32, (256, 256), 1) // 64
    averager = jnp.where(row == col, 1.0 / 64, 0.0).astype(BF16)
    squares = (x * x).astype(BF16)
    means = [matmul(squares[:, at : at + 256], averager) for at in range(0, x.shape[1], 256)]
    return x * lax.rsqrt(jnp.concatenate(means, axis=1) + EPSILON) * gain


def pair_of(x, p):
    return x[:, 128 * p : 128 * (p + 1)]


def attend(q, k, v):
    low = low_lanes(q.shape)
    values_low = low_lanes(v.shape)
    zero, one = jnp.zeros_like(q), jnp.ones_like(v)
    even = jnp.exp2(matmul_t(jnp.where(low, q, zero), k)).astype(BF16)
    odd = jnp.exp2(matmul_t(jnp.where(low, zero, q), k)).astype(BF16)
    even = matmul(even, jnp.where(values_low, v, one))
    odd = matmul(odd, jnp.where(values_low, one, v))
    return jnp.where(low, even, odd), jnp.where(low, odd, even)


def attend_whole(q, k, v):
    numerator, crossed = attend(q, k, v)
    return (numerator / pltpu.roll(crossed, 64, axis=1)).astype(BF16)


def hand_out(blocks_ref, outs):
    mine = own_pair()
    for k, out in enumerate(outs):
        out[...] = blocks_ref[mine ^ k]


def swap(x):
    return pltpu.roll(x, 64, axis=1)


def key_value_heads(keys, values):
    out = []
    for p in range(PAIRS):
        k, v = pair_of(keys, p), pair_of(values, p)
        low = low_lanes(k.shape)
        out.append(jnp.where(low, k, swap(v)).astype(BF16))
        out.append(jnp.where(low, swap(k), v).astype(BF16))
    return out


def query_heads(queries):
    half = queries.shape[0] // 2
    out = []
    for p in range(PAIRS):
        q = pair_of(queries, p)
        s = swap(q)
        low = low_lanes((half, 128))
        out.append(jnp.where(low, q[:half], s[half:]).astype(BF16))
        out.append(jnp.where(low, s[:half], q[half:]).astype(BF16))
    return out


def with_ones(kv, low):
    return jnp.where(low, jnp.ones_like(kv), kv)


def project_kernel(
    tokens_hbm,
    latents_hbm,
    wq_hbm,
    wkv_hbm,
    gain_hbm,
    send_ref,
    tokens_ref,
    latents_ref,
    wq_ref,
    wkv_ref,
    gain_ref,
    sems,
):
    half = wkv_ref.shape[1] // 2
    copies = [
        pltpu.make_async_copy(src, dst, sems.at[i])
        for i, (src, dst) in enumerate(
            (
                (gain_hbm, gain_ref),
                (latents_hbm, latents_ref),
                (tokens_hbm, tokens_ref),
                (wq_hbm, wq_ref),
                (wkv_hbm.at[:, :half], wkv_ref.at[:, :half]),
                (wkv_hbm.at[:, half:], wkv_ref.at[:, half:]),
            )
        )
    ]
    for copy in copies:
        copy.start()
    groups = send_ref.shape[0] // HEADS
    count = tokens_ref.shape[0] // groups
    copies[0].wait()
    copies[1].wait()
    latents = rms_rows(latents_ref[...].astype(F32))
    copies[2].wait()
    normed = rms_rows(tokens_ref[...].astype(F32))
    copies[3].wait()
    queries = head_norm(matmul(latents, wq_ref[...]), gain_ref[0:1, :] * QUERY_SCALE)
    for h, block in enumerate(query_heads(queries)):
        for g in range(groups):
            send_ref[g * HEADS + h, count:, :] = block
    copies[4].wait()
    keys = head_norm(matmul(normed, wkv_ref[:, :half]), gain_ref[1:2, :])
    copies[5].wait()
    values = matmul(normed, wkv_ref[:, half:])
    for h, block in enumerate(key_value_heads(keys, values)):
        for g in range(groups):
            send_ref[g * HEADS + h, :count, :] = block[g * count : (g + 1) * count]


def write_query_kernel(tokens_ref, wwq_ref, gain_ref, o0, o1, o2, o3, blocks_ref):
    normed = rms_rows(tokens_ref[...].astype(F32))
    queries = head_norm(matmul(normed, wwq_ref[...]), gain_ref[4:5, :] * QUERY_SCALE).astype(BF16)
    for p in range(PAIRS):
        blocks_ref[p] = pair_of(queries, p)
    hand_out(blocks_ref, (o0, o1, o2, o3))


def read_kernel(got_ref, out_ref):
    devices, rows, _ = got_ref.shape
    count = rows - 16
    kv = got_ref[:, :count, :].reshape(devices * count, 128)
    kv1 = with_ones(kv, low_lanes(kv.shape))
    step = 8
    for at in range(0, devices, step):
        packed = got_ref[at : at + step, count:, :].reshape(step * 16, 128).astype(F32)
        low = low_lanes(packed.shape)
        q = jnp.concatenate([packed, swap(packed)], axis=0)
        q = jnp.where(low_lanes(q.shape), q, 0.0).astype(BF16)
        o = matmul(jnp.exp2(matmul_t(q, kv)).astype(BF16), kv1)
        top, bottom = o[: step * 16], o[step * 16 :]
        numerators = jnp.where(low, swap(top), bottom)
        out_ref[at : at + step, :16] = numerators.astype(BF16).reshape(step, 16, 128)
        denominators = jnp.where(low, top, swap(bottom)).reshape(step, 2, 8, 128)
        part = lax.broadcasted_iota(jnp.int32, (step, 8, 128), 2) // 32 % 2
        denominators = jnp.where(part == 0, denominators[:, 0], denominators[:, 1])
        out_ref[at : at + step, 16:] = denominators.astype(BF16)


def unpacked_heads(got_ref):
    groups = got_ref.shape[0] // HEADS
    first = lax.broadcasted_iota(jnp.int32, (8, 128), 1) // 32 % 2 == 0
    heads = []
    for h in range(HEADS):
        total = got_ref[h].astype(F32)
        for g in range(1, groups):
            total = total + got_ref[g * HEADS + h].astype(F32)
        numerators, packed = total[:16], total[16:]
        top, bottom = jnp.where(first, packed, 0.0), jnp.where(first, 0.0, packed)
        top = top + pltpu.roll(top, 32, axis=1)
        bottom = bottom + pltpu.roll(bottom, 96, axis=1)
        heads.append(numerators / jnp.concatenate([top, bottom], axis=0))
    return heads


def self_project_kernel(
    got_ref, latents_ref, wo_ref, wqkv_ref, gain_ref, rows_ref, send_ref, q0, q1, q2, q3, blocks_ref
):
    devices = got_ref.shape[0]
    count = latents_ref.shape[0]
    attended = []
    heads = unpacked_heads(got_ref)
    low = low_lanes(heads[0].shape)
    for e, o in zip(heads[0::2], heads[1::2]):
        top, bottom = jnp.where(low, e, swap(o)), jnp.where(low, swap(e), o)
        attended.append(jnp.concatenate([top, bottom], axis=0).astype(BF16))
    attended = jnp.concatenate(attended, axis=1)
    rows = (latents_ref[...].astype(F32) + matmul(attended, wo_ref[...])).astype(BF16)
    rows_ref[...] = rows
    triple = matmul(rms_rows(rows.astype(F32)), wqkv_ref[...])
    queries = head_norm(triple[:, :512], gain_ref[2:3, :] * QUERY_SCALE).astype(BF16)
    keys = head_norm(triple[:, 512:1024], gain_ref[3:4, :]).astype(BF16)
    values = triple[:, 1024:].astype(BF16)
    for p in range(PAIRS):
        blocks_ref[p] = pair_of(queries, p)
    for d in range(devices):
        send_ref[d, :count] = pair_of(keys, d % PAIRS)
        send_ref[d, count:] = pair_of(values, d % PAIRS)
    hand_out(blocks_ref, (q0, q1, q2, q3))


def keys_of(got_ref):
    devices, rows, _ = got_ref.shape
    return got_ref[:, : rows // 2].reshape(devices * rows // 2, 128)


def values_of(got_ref):
    devices, rows, _ = got_ref.shape
    return got_ref[:, rows // 2 :].reshape(devices * rows // 2, 128)


def attend_kernel(got_ref, *refs):
    queries, outs = refs[: len(refs) // 2], refs[len(refs) // 2 :]
    count = queries[0].shape[0]
    q = jnp.concatenate([q[...] for q in queries], axis=0)
    result = attend_whole(q, keys_of(got_ref), values_of(got_ref))
    for i, out in enumerate(outs):
        out[...] = result[i * count : (i + 1) * count]


def gathered(blocks_ref, parts):
    mine = own_pair()
    for k, part in enumerate(parts):
        blocks_ref[mine ^ k] = part[...]
    return jnp.concatenate([blocks_ref[p] for p in range(PAIRS)], axis=1)


def write_project_kernel(
    a3, a2, a1, a0, rows_ref, wo_ref, wkv_ref, gain_ref, latents_ref, send_ref, blocks_ref
):
    attended = gathered(blocks_ref, (a0, a1, a2, a3))
    rows = (rows_ref[...].astype(F32) + matmul(attended, wo_ref[...])).astype(BF16)
    latents_ref[...] = rows
    count = rows.shape[0]
    kv = matmul(rms_rows(rows.astype(F32)), wkv_ref[...])
    keys = head_norm(kv[:, :512], gain_ref[5:6, :]).astype(BF16)
    values = kv[:, 512:].astype(BF16)
    for d in range(send_ref.shape[0]):
        send_ref[d, :count] = pair_of(keys, d % PAIRS)
        send_ref[d, count:] = pair_of(values, d % PAIRS)


def finish_kernel(a0, a1, a2, a3, tokens_ref, wo_ref, out_ref, blocks_ref):
    update = matmul(gathered(blocks_ref, (a0, a1, a2, a3)), wo_ref[...])
    out_ref[...] = (tokens_ref[...].astype(F32) + update).astype(BF16)


def call(body, outs, *args, scratch=(), fetch=None):
    space = pltpu.HBM if fetch else pltpu.VMEM
    scratch = list(scratch)
    if fetch:
        scratch += [pltpu.VMEM(a.shape, a.dtype) for a in args]
        scratch.append(pltpu.SemaphoreType.DMA((len(args) + fetch,)))
        args = [pltpu.with_memory_space_constraint(a, space) for a in args]
    results = pl.pallas_call(
        body,
        out_shape=tuple(jax.ShapeDtypeStruct(s, BF16) for s in outs),
        in_specs=[pl.BlockSpec(memory_space=space)] * len(args),
        out_specs=tuple(pl.BlockSpec(memory_space=pltpu.VMEM) for _ in outs),
        scratch_shapes=scratch,
        compiler_params=pltpu.CompilerParams(vmem_limit_bytes=48 * 1024 * 1024),
        cost_estimate=pl.CostEstimate(
            flops=10**9,
            transcendentals=0,
            bytes_accessed=sum(a.size * a.dtype.itemsize for a in args),
        ),
    )(*args)
    return results if len(outs) > 1 else results[0]


def blocks(rows):
    return [pltpu.VMEM((PAIRS, rows, 128), BF16)]


def all_to_all(x):
    return lax.all_to_all(x, AA, split_axis=0, concat_axis=0, tiled=True)


def swapped(parts):
    return tuple(to_peer(parts[k], k) for k in (3, 2, 1)) + (parts[0],)


def layer(
    tokens,
    latents,
    read_query,
    read_keyval,
    read_out,
    self_qkv,
    self_out,
    write_query,
    write_keyval,
    write_out,
    qk_gain,
):
    count, rows = tokens.shape[0], latents.shape[0]
    devices = lax.axis_size(AA)
    sent = call(
        project_kernel,
        ((devices, count * HEADS // devices + 16, 128),),
        tokens,
        latents,
        read_query,
        read_keyval,
        qk_gain,
        fetch=1,
    )
    partial = call(read_kernel, ((devices, 24, 128),), all_to_all(sent))
    own_rows, sent, *queries = call(
        self_project_kernel,
        ((rows, 1024), (devices, 2 * rows, 128)) + ((rows, 128),) * 4,
        all_to_all(partial),
        latents,
        read_out,
        self_qkv,
        qk_gain,
        scratch=blocks(rows),
    )
    asked = call(
        write_query_kernel,
        ((count, 128),) * 4,
        tokens,
        write_query,
        qk_gain,
        scratch=blocks(count),
    )
    q3, q2, q1, q0 = swapped(asked)
    got = all_to_all(sent)
    queries = swapped(queries)
    attended = call(attend_kernel, ((rows, 128),) * 4, got, *queries)[::-1]
    latents_out, sent = call(
        write_project_kernel,
        ((rows, 1024), (devices, 2 * rows, 128)),
        *swapped(attended),
        own_rows,
        self_out,
        write_keyval,
        qk_gain,
        scratch=blocks(rows),
    )
    sent, q3, q2, q1, q0 = lax.optimization_barrier((sent, q3, q2, q1, q0))
    got = all_to_all(sent)
    a3, a2 = call(attend_kernel, ((count, 128),) * 2, got, q3, q2)
    a3, a2 = to_peer(a3, 3), to_peer(a2, 2)
    a1 = to_peer(call(attend_kernel, ((count, 128),), got, q1), 1)
    a0 = call(attend_kernel, ((count, 128),), got, q0)
    tokens_out = call(
        finish_kernel,
        ((count, 1024),),
        a0,
        a1,
        a2,
        a3,
        tokens,
        write_out,
        scratch=blocks(count),
    )
    return (tokens_out, latents_out)


def solution(mesh):
    torus = Mesh(mesh.devices.reshape(mesh.shape["ba"], 4, 4, 2), ("ba", "aa_0", "aa_1", "aa_2"))
    in_specs = (P(BA_AA, None), P(BA_AA, None), P(), P(), P(), P(), P(), P(), P(), P(), P())
    out_specs = (P(BA_AA, None), P(BA_AA, None))
    return jax.shard_map(layer, mesh=torus, in_specs=in_specs, out_specs=out_specs, check_vma=False)
```

```python
import math

import jax
import jax.numpy as jnp
from jax import lax
from jax.experimental import pallas as pl
from jax.experimental.pallas import tpu as pltpu
from jax.sharding import Mesh
from jax.sharding import PartitionSpec as P


AA = ("aa_0", "aa_1", "aa_2")
BA_AA = ("ba", "aa_0", "aa_1", "aa_2")
HEADS = 8
PAIRS = 4
EPSILON = 1e-06
QUERY_SCALE = math.log2(math.e) / 8.0
F32, BF16 = jnp.float32, jnp.bfloat16


def own_pair():
    return 2 * lax.rem(lax.axis_index("aa_1"), 2) + lax.axis_index("aa_2")


def to_peer(x, k):
    swaps = [(i, i ^ k) for i in range(8)]
    return lax.ppermute(x, ("aa_1", "aa_2"), swaps)


def low_lanes(shape):
    return lax.broadcasted_iota(jnp.int32, shape, len(shape) - 1) < 64


def rms_rows(x):
    return (x * lax.rsqrt(jnp.mean(x * x, axis=-1, keepdims=True) + EPSILON)).astype(BF16)


def matmul(a, b):
    return jnp.dot(a, b, preferred_element_type=F32)


def matmul_t(a, b):
    return lax.dot_general(a, b, (((1,), (1,)), ((), ())), preferred_element_type=F32)


def head_norm(x, gain):
    row = lax.broadcasted_iota(jnp.int32, (256, 256), 0) // 64
    col = lax.broadcasted_iota(jnp.int32, (256, 256), 1) // 64
    averager = jnp.where(row == col, 1.0 / 64, 0.0).astype(BF16)
    squares = (x * x).astype(BF16)
    means = [matmul(squares[:, at : at + 256], averager) for at in range(0, x.shape[1], 256)]
    return x * lax.rsqrt(jnp.concatenate(means, axis=1) + EPSILON) * gain


def pair_of(x, p):
    return x[:, 128 * p : 128 * (p + 1)]


def attend(q, k, v):
    low = low_lanes(q.shape)
    values_low = low_lanes(v.shape)
    zero, one = jnp.zeros_like(q), jnp.ones_like(v)
    even = jnp.exp2(matmul_t(jnp.where(low, q, zero), k)).astype(BF16)
    odd = jnp.exp2(matmul_t(jnp.where(low, zero, q), k)).astype(BF16)
    even = matmul(even, jnp.where(values_low, v, one))
    odd = matmul(odd, jnp.where(values_low, one, v))
    return jnp.where(low, even, odd), jnp.where(low, odd, even)


def attend_whole(q, k, v):
    numerator, crossed = attend(q, k, v)
    return (numerator / pltpu.roll(crossed, 64, axis=1)).astype(BF16)


def hand_out(blocks_ref, outs):
    mine = own_pair()
    for k, out in enumerate(outs):
        out[...] = blocks_ref[mine ^ k]


def swap(x):
    return pltpu.roll(x, 64, axis=1)


def key_value_heads(keys, values):
    out = []
    for p in range(PAIRS):
        k, v = pair_of(keys, p), pair_of(values, p)
        low = low_lanes(k.shape)
        out.append(jnp.where(low, k, swap(v)).astype(BF16))
        out.append(jnp.where(low, swap(k), v).astype(BF16))
    return out


def query_heads(queries):
    half = queries.shape[0] // 2
    out = []
    for p in range(PAIRS):
        q = pair_of(queries, p)
        s = swap(q)
        low = low_lanes((half, 128))
        out.append(jnp.where(low, q[:half], s[half:]).astype(BF16))
        out.append(jnp.where(low, s[:half], q[half:]).astype(BF16))
    return out


def with_ones(kv, low):
    return jnp.where(low, jnp.ones_like(kv), kv)


def project_kernel(
    tokens_hbm,
    latents_hbm,
    wq_hbm,
    wkv_hbm,
    gain_hbm,
    send_ref,
    tokens_ref,
    latents_ref,
    wq_ref,
    wkv_ref,
    gain_ref,
    sems,
):
    half = wkv_ref.shape[1] // 2
    copies = [
        pltpu.make_async_copy(src, dst, sems.at[i])
        for i, (src, dst) in enumerate(
            (
                (gain_hbm, gain_ref),
                (latents_hbm, latents_ref),
                (tokens_hbm, tokens_ref),
                (wq_hbm, wq_ref),
                (wkv_hbm.at[:, :half], wkv_ref.at[:, :half]),
                (wkv_hbm.at[:, half:], wkv_ref.at[:, half:]),
            )
        )
    ]
    for copy in copies:
        copy.start()
    groups = send_ref.shape[0] // HEADS
    count = tokens_ref.shape[0] // groups
    copies[0].wait()
    copies[1].wait()
    latents = rms_rows(latents_ref[...].astype(F32))
    copies[2].wait()
    normed = rms_rows(tokens_ref[...].astype(F32))
    copies[3].wait()
    queries = head_norm(matmul(latents, wq_ref[...]), gain_ref[0:1, :] * QUERY_SCALE)
    for h, block in enumerate(query_heads(queries)):
        for g in range(groups):
            send_ref[g * HEADS + h, count:, :] = block
    copies[4].wait()
    keys = head_norm(matmul(normed, wkv_ref[:, :half]), gain_ref[1:2, :])
    copies[5].wait()
    values = matmul(normed, wkv_ref[:, half:])
    for h, block in enumerate(key_value_heads(keys, values)):
        for g in range(groups):
            send_ref[g * HEADS + h, :count, :] = block[g * count : (g + 1) * count]


def write_query_kernel(tokens_ref, wwq_ref, gain_ref, o0, o1, o2, o3, blocks_ref):
    normed = rms_rows(tokens_ref[...].astype(F32))
    queries = head_norm(matmul(normed, wwq_ref[...]), gain_ref[4:5, :] * QUERY_SCALE).astype(BF16)
    for p in range(PAIRS):
        blocks_ref[p] = pair_of(queries, p)
    hand_out(blocks_ref, (o0, o1, o2, o3))


def read_kernel(got_ref, out_ref):
    devices, rows, _ = got_ref.shape
    count = rows - 16
    kv = got_ref[:, :count, :].reshape(devices * count, 128)
    kv1 = with_ones(kv, low_lanes(kv.shape))
    step = 8
    for at in range(0, devices, step):
        packed = got_ref[at : at + step, count:, :].reshape(step * 16, 128).astype(F32)
        low = low_lanes(packed.shape)
        q = jnp.concatenate([packed, swap(packed)], axis=0)
        q = jnp.where(low_lanes(q.shape), q, 0.0).astype(BF16)
        o = matmul(jnp.exp2(matmul_t(q, kv)).astype(BF16), kv1)
        top, bottom = o[: step * 16], o[step * 16 :]
        numerators = jnp.where(low, swap(top), bottom)
        out_ref[at : at + step, :16] = numerators.astype(BF16).reshape(step, 16, 128)
        denominators = jnp.where(low, top, swap(bottom)).reshape(step, 2, 8, 128)
        part = lax.broadcasted_iota(jnp.int32, (step, 8, 128), 2) // 32 % 2
        denominators = jnp.where(part == 0, denominators[:, 0], denominators[:, 1])
        out_ref[at : at + step, 16:] = denominators.astype(BF16)


def unpacked_heads(got_ref):
    groups = got_ref.shape[0] // HEADS
    first = lax.broadcasted_iota(jnp.int32, (8, 128), 1) // 32 % 2 == 0
    heads = []
    for h in range(HEADS):
        total = got_ref[h].astype(F32)
        for g in range(1, groups):
            total = total + got_ref[g * HEADS + h].astype(F32)
        numerators, packed = total[:16], total[16:]
        top, bottom = jnp.where(first, packed, 0.0), jnp.where(first, 0.0, packed)
        top = top + pltpu.roll(top, 32, axis=1)
        bottom = bottom + pltpu.roll(bottom, 96, axis=1)
        heads.append(numerators / jnp.concatenate([top, bottom], axis=0))
    return heads


def self_project_kernel(
    got_ref, latents_ref, wo_ref, wqkv_ref, gain_ref, rows_ref, send_ref
):
    devices = got_ref.shape[0]
    count = latents_ref.shape[0]
    attended = []
    heads = unpacked_heads(got_ref)
    low = low_lanes(heads[0].shape)
    for e, o in zip(heads[0::2], heads[1::2]):
        top, bottom = jnp.where(low, e, swap(o)), jnp.where(low, swap(e), o)
        attended.append(jnp.concatenate([top, bottom], axis=0).astype(BF16))
    attended = jnp.concatenate(attended, axis=1)
    rows = (latents_ref[...].astype(F32) + matmul(attended, wo_ref[...])).astype(BF16)
    rows_ref[...] = rows
    pairs = matmul(rms_rows(rows.astype(F32)), wqkv_ref[:, 512:])
    keys = head_norm(pairs[:, :512], gain_ref[3:4, :]).astype(BF16)
    values = pairs[:, 512:].astype(BF16)
    for d in range(devices):
        send_ref[d, :count] = pair_of(keys, d % PAIRS)
        send_ref[d, count:] = pair_of(values, d % PAIRS)


def self_query_kernel(rows_ref, wqkv_ref, gain_ref, o0, o1, o2, o3, blocks_ref):
    normed = rms_rows(rows_ref[...].astype(F32))
    queries = matmul(normed, wqkv_ref[:, :512])
    queries = head_norm(queries, gain_ref[2:3, :] * QUERY_SCALE).astype(BF16)
    for p in range(PAIRS):
        blocks_ref[p] = pair_of(queries, p)
    hand_out(blocks_ref, (o0, o1, o2, o3))


def keys_of(got_ref):
    devices, rows, _ = got_ref.shape
    return got_ref[:, : rows // 2].reshape(devices * rows // 2, 128)


def values_of(got_ref):
    devices, rows, _ = got_ref.shape
    return got_ref[:, rows // 2 :].reshape(devices * rows // 2, 128)


def attend_kernel(got_ref, *refs):
    queries, outs = refs[: len(refs) // 2], refs[len(refs) // 2 :]
    count = queries[0].shape[0]
    q = jnp.concatenate([q[...] for q in queries], axis=0)
    result = attend_whole(q, keys_of(got_ref), values_of(got_ref))
    for i, out in enumerate(outs):
        out[...] = result[i * count : (i + 1) * count]


def gathered(blocks_ref, parts):
    mine = own_pair()
    for k, part in enumerate(parts):
        blocks_ref[mine ^ k] = part[...]
    return jnp.concatenate([blocks_ref[p] for p in range(PAIRS)], axis=1)


def write_project_kernel(
    a3, a2, a1, a0, rows_ref, wo_ref, wkv_ref, gain_ref, latents_ref, send_ref, blocks_ref
):
    attended = gathered(blocks_ref, (a0, a1, a2, a3))
    rows = (rows_ref[...].astype(F32) + matmul(attended, wo_ref[...])).astype(BF16)
    latents_ref[...] = rows
    count = rows.shape[0]
    kv = matmul(rms_rows(rows.astype(F32)), wkv_ref[...])
    keys = head_norm(kv[:, :512], gain_ref[5:6, :]).astype(BF16)
    values = kv[:, 512:].astype(BF16)
    for d in range(send_ref.shape[0]):
        send_ref[d, :count] = pair_of(keys, d % PAIRS)
        send_ref[d, count:] = pair_of(values, d % PAIRS)


def finish_kernel(a0, a1, a2, a3, tokens_ref, wo_ref, out_ref, blocks_ref):
    update = matmul(gathered(blocks_ref, (a0, a1, a2, a3)), wo_ref[...])
    out_ref[...] = (tokens_ref[...].astype(F32) + update).astype(BF16)


def call(body, outs, *args, scratch=(), fetch=None):
    space = pltpu.HBM if fetch else pltpu.VMEM
    scratch = list(scratch)
    if fetch:
        scratch += [pltpu.VMEM(a.shape, a.dtype) for a in args]
        scratch.append(pltpu.SemaphoreType.DMA((len(args) + fetch,)))
        args = [pltpu.with_memory_space_constraint(a, space) for a in args]
    results = pl.pallas_call(
        body,
        out_shape=tuple(jax.ShapeDtypeStruct(s, BF16) for s in outs),
        in_specs=[pl.BlockSpec(memory_space=space)] * len(args),
        out_specs=tuple(pl.BlockSpec(memory_space=pltpu.VMEM) for _ in outs),
        scratch_shapes=scratch,
        compiler_params=pltpu.CompilerParams(vmem_limit_bytes=48 * 1024 * 1024),
        cost_estimate=pl.CostEstimate(
            flops=10**9,
            transcendentals=0,
            bytes_accessed=sum(a.size * a.dtype.itemsize for a in args),
        ),
    )(*args)
    return results if len(outs) > 1 else results[0]


def blocks(rows):
    return [pltpu.VMEM((PAIRS, rows, 128), BF16)]


def all_to_all(x):
    return lax.all_to_all(x, AA, split_axis=0, concat_axis=0, tiled=True)


def swapped(parts):
    return tuple(to_peer(parts[k], k) for k in (3, 2, 1)) + (parts[0],)


def layer(
    tokens,
    latents,
    read_query,
    read_keyval,
    read_out,
    self_qkv,
    self_out,
    write_query,
    write_keyval,
    write_out,
    qk_gain,
):
    count, rows = tokens.shape[0], latents.shape[0]
    devices = lax.axis_size(AA)
    sent = call(
        project_kernel,
        ((devices, count * HEADS // devices + 16, 128),),
        tokens,
        latents,
        read_query,
        read_keyval,
        qk_gain,
        fetch=1,
    )
    partial = call(read_kernel, ((devices, 24, 128),), all_to_all(sent))
    own_rows, sent = call(
        self_project_kernel,
        ((rows, 1024), (devices, 2 * rows, 128)),
        all_to_all(partial),
        latents,
        read_out,
        self_qkv,
        qk_gain,
    )
    queries = call(
        self_query_kernel,
        ((rows, 128),) * 4,
        own_rows,
        self_qkv,
        qk_gain,
        scratch=blocks(rows),
    )
    asked = call(
        write_query_kernel,
        ((count, 128),) * 4,
        tokens,
        write_query,
        qk_gain,
        scratch=blocks(count),
    )
    q3, q2, q1, q0 = swapped(asked)
    got = all_to_all(sent)
    queries = swapped(queries)
    attended = call(attend_kernel, ((rows, 128),) * 4, got, *queries)[::-1]
    latents_out, sent = call(
        write_project_kernel,
        ((rows, 1024), (devices, 2 * rows, 128)),
        *swapped(attended),
        own_rows,
        self_out,
        write_keyval,
        qk_gain,
        scratch=blocks(rows),
    )
    sent, q3, q2, q1, q0 = lax.optimization_barrier((sent, q3, q2, q1, q0))
    got = all_to_all(sent)
    a3, a2 = call(attend_kernel, ((count, 128),) * 2, got, q3, q2)
    a3, a2 = to_peer(a3, 3), to_peer(a2, 2)
    a1 = to_peer(call(attend_kernel, ((count, 128),), got, q1), 1)
    a0 = call(attend_kernel, ((count, 128),), got, q0)
    tokens_out = call(
        finish_kernel,
        ((count, 1024),),
        a0,
        a1,
        a2,
        a3,
        tokens,
        write_out,
        scratch=blocks(count),
    )
    return (tokens_out, latents_out)


def solution(mesh):
    torus = Mesh(mesh.devices.reshape(mesh.shape["ba"], 4, 4, 2), ("ba", "aa_0", "aa_1", "aa_2"))
    in_specs = (P(BA_AA, None), P(BA_AA, None), P(), P(), P(), P(), P(), P(), P(), P(), P())
    out_specs = (P(BA_AA, None), P(BA_AA, None))
    return jax.shard_map(layer, mesh=torus, in_specs=in_specs, out_specs=out_specs, check_vma=False)
```

```python
import math

import jax
import jax.numpy as jnp
from jax import lax
from jax.experimental import pallas as pl
from jax.experimental.pallas import tpu as pltpu
from jax.sharding import Mesh
from jax.sharding import PartitionSpec as P


AA = ("aa_0", "aa_1", "aa_2")
BA_AA = ("ba", "aa_0", "aa_1", "aa_2")
HEADS = 8
PAIRS = 4
EPSILON = 1e-06
QUERY_SCALE = math.log2(math.e) / 8.0
F32, BF16 = jnp.float32, jnp.bfloat16


def own_pair():
    return 2 * lax.rem(lax.axis_index("aa_1"), 2) + lax.axis_index("aa_2")


def to_peer(x, k):
    swaps = [(i, i ^ k) for i in range(8)]
    return lax.ppermute(x, ("aa_1", "aa_2"), swaps)


def low_lanes(shape):
    return lax.broadcasted_iota(jnp.int32, shape, len(shape) - 1) < 64


def rms_rows(x):
    return (x * lax.rsqrt(jnp.mean(x * x, axis=-1, keepdims=True) + EPSILON)).astype(BF16)


def matmul(a, b):
    return jnp.dot(a, b, preferred_element_type=F32)


def matmul_t(a, b):
    return lax.dot_general(a, b, (((1,), (1,)), ((), ())), preferred_element_type=F32)


def head_norm(x, gain):
    row = lax.broadcasted_iota(jnp.int32, (256, 256), 0) // 64
    col = lax.broadcasted_iota(jnp.int32, (256, 256), 1) // 64
    averager = jnp.where(row == col, 1.0 / 64, 0.0).astype(BF16)
    squares = (x * x).astype(BF16)
    means = [matmul(squares[:, at : at + 256], averager) for at in range(0, x.shape[1], 256)]
    return x * lax.rsqrt(jnp.concatenate(means, axis=1) + EPSILON) * gain


def pair_of(x, p):
    return x[:, 128 * p : 128 * (p + 1)]


def attend(q, k, v):
    low = low_lanes(q.shape)
    values_low = low_lanes(v.shape)
    zero, one = jnp.zeros_like(q), jnp.ones_like(v)
    even = jnp.exp2(matmul_t(jnp.where(low, q, zero), k)).astype(BF16)
    odd = jnp.exp2(matmul_t(jnp.where(low, zero, q), k)).astype(BF16)
    even = matmul(even, jnp.where(values_low, v, one))
    odd = matmul(odd, jnp.where(values_low, one, v))
    return jnp.where(low, even, odd), jnp.where(low, odd, even)


def attend_whole(q, k, v):
    numerator, crossed = attend(q, k, v)
    return (numerator / pltpu.roll(crossed, 64, axis=1)).astype(BF16)


def hand_out(blocks_ref, outs):
    mine = own_pair()
    for k, out in enumerate(outs):
        out[...] = blocks_ref[mine ^ k]


def swap(x):
    return pltpu.roll(x, 64, axis=1)


def key_value_heads(keys, values):
    out = []
    for p in range(PAIRS):
        k, v = pair_of(keys, p), pair_of(values, p)
        low = low_lanes(k.shape)
        out.append(jnp.where(low, k, swap(v)).astype(BF16))
        out.append(jnp.where(low, swap(k), v).astype(BF16))
    return out


def query_heads(queries):
    half = queries.shape[0] // 2
    out = []
    for p in range(PAIRS):
        q = pair_of(queries, p)
        s = swap(q)
        low = low_lanes((half, 128))
        out.append(jnp.where(low, q[:half], s[half:]).astype(BF16))
        out.append(jnp.where(low, s[:half], q[half:]).astype(BF16))
    return out


def with_ones(kv, low):
    return jnp.where(low, jnp.ones_like(kv), kv)


def project_kernel(
    tokens_hbm,
    latents_hbm,
    wq_hbm,
    wkv_hbm,
    gain_hbm,
    send_ref,
    tokens_ref,
    latents_ref,
    wq_ref,
    wkv_ref,
    gain_ref,
    sems,
):
    half = wkv_ref.shape[1] // 2
    copies = [
        pltpu.make_async_copy(src, dst, sems.at[i])
        for i, (src, dst) in enumerate(
            (
                (gain_hbm, gain_ref),
                (latents_hbm, latents_ref),
                (tokens_hbm, tokens_ref),
                (wq_hbm, wq_ref),
                (wkv_hbm.at[:, :half], wkv_ref.at[:, :half]),
                (wkv_hbm.at[:, half:], wkv_ref.at[:, half:]),
            )
        )
    ]
    for copy in copies:
        copy.start()
    groups = send_ref.shape[0] // HEADS
    count = tokens_ref.shape[0] // groups
    copies[0].wait()
    copies[1].wait()
    latents = rms_rows(latents_ref[...].astype(F32))
    copies[2].wait()
    normed = rms_rows(tokens_ref[...].astype(F32))
    copies[3].wait()
    queries = head_norm(matmul(latents, wq_ref[...]), gain_ref[0:1, :] * QUERY_SCALE)
    for h, block in enumerate(query_heads(queries)):
        for g in range(groups):
            send_ref[g * HEADS + h, count:, :] = block
    copies[4].wait()
    keys = head_norm(matmul(normed, wkv_ref[:, :half]), gain_ref[1:2, :])
    copies[5].wait()
    values = matmul(normed, wkv_ref[:, half:])
    for h, block in enumerate(key_value_heads(keys, values)):
        for g in range(groups):
            send_ref[g * HEADS + h, :count, :] = block[g * count : (g + 1) * count]


def write_query_kernel(tokens_ref, wwq_ref, gain_ref, o0, o1, o2, o3, blocks_ref):
    normed = rms_rows(tokens_ref[...].astype(F32))
    queries = head_norm(matmul(normed, wwq_ref[...]), gain_ref[4:5, :] * QUERY_SCALE).astype(BF16)
    for p in range(PAIRS):
        blocks_ref[p] = pair_of(queries, p)
    hand_out(blocks_ref, (o0, o1, o2, o3))


def read_kernel(got_ref, out_ref):
    devices, rows, _ = got_ref.shape
    count = rows - 16
    kv = got_ref[:, :count, :].reshape(devices * count, 128)
    kv1 = with_ones(kv, low_lanes(kv.shape))
    step = 16
    for at in range(0, devices, step):
        packed = got_ref[at : at + step, count:, :].reshape(step * 16, 128).astype(F32)
        low = low_lanes(packed.shape)
        q = jnp.concatenate([packed, swap(packed)], axis=0)
        q = jnp.where(low_lanes(q.shape), q, 0.0).astype(BF16)
        o = matmul(jnp.exp2(matmul_t(q, kv)).astype(BF16), kv1)
        top, bottom = o[: step * 16], o[step * 16 :]
        numerators = jnp.where(low, swap(top), bottom)
        out_ref[at : at + step, :16] = numerators.astype(BF16).reshape(step, 16, 128)
        denominators = jnp.where(low, top, swap(bottom)).reshape(step, 2, 8, 128)
        part = lax.broadcasted_iota(jnp.int32, (step, 8, 128), 2) // 32 % 2
        denominators = jnp.where(part == 0, denominators[:, 0], denominators[:, 1])
        out_ref[at : at + step, 16:] = denominators.astype(BF16)


def unpacked_heads(got_ref):
    groups = got_ref.shape[0] // HEADS
    first = lax.broadcasted_iota(jnp.int32, (8, 128), 1) // 32 % 2 == 0
    heads = []
    for h in range(HEADS):
        total = got_ref[h].astype(F32)
        for g in range(1, groups):
            total = total + got_ref[g * HEADS + h].astype(F32)
        numerators, packed = total[:16], total[16:]
        top, bottom = jnp.where(first, packed, 0.0), jnp.where(first, 0.0, packed)
        top = top + pltpu.roll(top, 32, axis=1)
        bottom = bottom + pltpu.roll(bottom, 96, axis=1)
        heads.append(numerators / jnp.concatenate([top, bottom], axis=0))
    return heads


def self_project_kernel(
    got_ref, latents_ref, wo_ref, wqkv_ref, gain_ref, rows_ref, send_ref
):
    devices = got_ref.shape[0]
    count = latents_ref.shape[0]
    attended = []
    heads = unpacked_heads(got_ref)
    low = low_lanes(heads[0].shape)
    for e, o in zip(heads[0::2], heads[1::2]):
        top, bottom = jnp.where(low, e, swap(o)), jnp.where(low, swap(e), o)
        attended.append(jnp.concatenate([top, bottom], axis=0).astype(BF16))
    attended = jnp.concatenate(attended, axis=1)
    rows = (latents_ref[...].astype(F32) + matmul(attended, wo_ref[...])).astype(BF16)
    rows_ref[...] = rows
    pairs = matmul(rms_rows(rows.astype(F32)), wqkv_ref[:, 512:])
    keys = head_norm(pairs[:, :512], gain_ref[3:4, :]).astype(BF16)
    values = pairs[:, 512:].astype(BF16)
    for d in range(devices):
        send_ref[d, :count] = pair_of(keys, d % PAIRS)
        send_ref[d, count:] = pair_of(values, d % PAIRS)


def self_query_kernel(
    rows_ref, wqkv_hbm, gain_ref, o0, o1, o2, o3, blocks_ref, wq_ref, sems
):
    copy = pltpu.make_async_copy(wqkv_hbm.at[:, :512], wq_ref, sems.at[0])
    copy.start()
    normed = rms_rows(rows_ref[...].astype(F32))
    copy.wait()
    queries = matmul(normed, wq_ref[...])
    queries = head_norm(queries, gain_ref[2:3, :] * QUERY_SCALE).astype(BF16)
    for p in range(PAIRS):
        blocks_ref[p] = pair_of(queries, p)
    hand_out(blocks_ref, (o0, o1, o2, o3))


def keys_of(got_ref):
    devices, rows, _ = got_ref.shape
    return got_ref[:, : rows // 2].reshape(devices * rows // 2, 128)


def values_of(got_ref):
    devices, rows, _ = got_ref.shape
    return got_ref[:, rows // 2 :].reshape(devices * rows // 2, 128)


def attend_kernel(got_ref, *refs):
    queries, outs = refs[: len(refs) // 2], refs[len(refs) // 2 :]
    count = queries[0].shape[0]
    q = jnp.concatenate([q[...] for q in queries], axis=0)
    result = attend_whole(q, keys_of(got_ref), values_of(got_ref))
    for i, out in enumerate(outs):
        out[...] = result[i * count : (i + 1) * count]


def gathered(blocks_ref, parts):
    mine = own_pair()
    for k, part in enumerate(parts):
        blocks_ref[mine ^ k] = part[...]
    return jnp.concatenate([blocks_ref[p] for p in range(PAIRS)], axis=1)


def write_project_kernel(
    a3, a2, a1, a0, rows_ref, wo_ref, wkv_ref, gain_ref, latents_ref, send_ref, blocks_ref
):
    attended = gathered(blocks_ref, (a0, a1, a2, a3))
    rows = (rows_ref[...].astype(F32) + matmul(attended, wo_ref[...])).astype(BF16)
    latents_ref[...] = rows
    count = rows.shape[0]
    kv = matmul(rms_rows(rows.astype(F32)), wkv_ref[...])
    keys = head_norm(kv[:, :512], gain_ref[5:6, :]).astype(BF16)
    values = kv[:, 512:].astype(BF16)
    for d in range(send_ref.shape[0]):
        send_ref[d, :count] = pair_of(keys, d % PAIRS)
        send_ref[d, count:] = pair_of(values, d % PAIRS)


def finish_kernel(a0, a1, a2, a3, tokens_ref, wo_ref, out_ref, blocks_ref):
    update = matmul(gathered(blocks_ref, (a0, a1, a2, a3)), wo_ref[...])
    out_ref[...] = (tokens_ref[...].astype(F32) + update).astype(BF16)


def call(body, outs, *args, scratch=(), fetch=None, far=()):
    space = pltpu.HBM if fetch else pltpu.VMEM
    scratch = list(scratch)
    if fetch:
        scratch += [pltpu.VMEM(a.shape, a.dtype) for a in args]
        scratch.append(pltpu.SemaphoreType.DMA((len(args) + fetch,)))
        args = [pltpu.with_memory_space_constraint(a, space) for a in args]
    args = [
        pltpu.with_memory_space_constraint(a, pltpu.HBM) if i in far else a
        for i, a in enumerate(args)
    ]
    results = pl.pallas_call(
        body,
        out_shape=tuple(jax.ShapeDtypeStruct(s, BF16) for s in outs),
        in_specs=[
            pl.BlockSpec(memory_space=pltpu.HBM if i in far else space) for i in range(len(args))
        ],
        out_specs=tuple(pl.BlockSpec(memory_space=pltpu.VMEM) for _ in outs),
        scratch_shapes=scratch,
        compiler_params=pltpu.CompilerParams(vmem_limit_bytes=48 * 1024 * 1024),
        cost_estimate=pl.CostEstimate(
            flops=10**9,
            transcendentals=0,
            bytes_accessed=sum(a.size * a.dtype.itemsize for a in args),
        ),
    )(*args)
    return results if len(outs) > 1 else results[0]


def blocks(rows):
    return [pltpu.VMEM((PAIRS, rows, 128), BF16)]


def all_to_all(x):
    return lax.all_to_all(x, AA, split_axis=0, concat_axis=0, tiled=True)


def swapped(parts):
    return tuple(to_peer(parts[k], k) for k in (3, 2, 1)) + (parts[0],)


def layer(
    tokens,
    latents,
    read_query,
    read_keyval,
    read_out,
    self_qkv,
    self_out,
    write_query,
    write_keyval,
    write_out,
    qk_gain,
):
    count, rows = tokens.shape[0], latents.shape[0]
    devices = lax.axis_size(AA)
    sent = call(
        project_kernel,
        ((devices, count * HEADS // devices + 16, 128),),
        tokens,
        latents,
        read_query,
        read_keyval,
        qk_gain,
        fetch=1,
    )
    partial = call(read_kernel, ((devices, 24, 128),), all_to_all(sent))
    own_rows, sent = call(
        self_project_kernel,
        ((rows, 1024), (devices, 2 * rows, 128)),
        all_to_all(partial),
        latents,
        read_out,
        self_qkv,
        qk_gain,
    )
    queries = call(
        self_query_kernel,
        ((rows, 128),) * 4,
        own_rows,
        self_qkv,
        qk_gain,
        scratch=blocks(rows)
        + [pltpu.VMEM((1024, 512), BF16), pltpu.SemaphoreType.DMA((1,))],
        far=(1,),
    )
    asked = call(
        write_query_kernel,
        ((count, 128),) * 4,
        tokens,
        write_query,
        qk_gain,
        scratch=blocks(count),
    )
    q3, q2, q1, q0 = swapped(asked)
    got = all_to_all(sent)
    queries = swapped(queries)
    attended = call(attend_kernel, ((rows, 128),) * 4, got, *queries)[::-1]
    latents_out, sent = call(
        write_project_kernel,
        ((rows, 1024), (devices, 2 * rows, 128)),
        *swapped(attended),
        own_rows,
        self_out,
        write_keyval,
        qk_gain,
        scratch=blocks(rows),
    )
    sent, q3, q2, q1, q0 = lax.optimization_barrier((sent, q3, q2, q1, q0))
    got = all_to_all(sent)
    a3, a2 = call(attend_kernel, ((count, 128),) * 2, got, q3, q2)
    a3, a2 = to_peer(a3, 3), to_peer(a2, 2)
    a1 = to_peer(call(attend_kernel, ((count, 128),), got, q1), 1)
    a0 = call(attend_kernel, ((count, 128),), got, q0)
    tokens_out = call(
        finish_kernel,
        ((count, 1024),),
        a0,
        a1,
        a2,
        a3,
        tokens,
        write_out,
        scratch=blocks(count),
    )
    return (tokens_out, latents_out)


def solution(mesh):
    torus = Mesh(mesh.devices.reshape(mesh.shape["ba"], 4, 4, 2), ("ba", "aa_0", "aa_1", "aa_2"))
    in_specs = (P(BA_AA, None), P(BA_AA, None), P(), P(), P(), P(), P(), P(), P(), P(), P())
    out_specs = (P(BA_AA, None), P(BA_AA, None))
    return jax.shard_map(layer, mesh=torus, in_specs=in_specs, out_specs=out_specs, check_vma=False)
```
